32 devices in a mesh: row: 4 (over y, x), col: 8 (over z, core).
Axes of the slice: x: 2, y: 2, z: 4, core: 2. Of those that a mesh axis runs over, the one named last changes fastest.
Arguments:
- basis: bfloat16 [40, 131072], P(None, ('row', 'col'))
- expand: float32 [3, 8, 40], replicated, may hold values from -1 to 1
- tiles: bfloat16 [3, 3072, 128, 128], P(None, ('row', 'col')), may hold values from -0.3125 to 0.3125
- tile_rows: int32 [3072], P(('row', 'col')), may hold values from 0 to 255, as said below
- tile_cols: int32 [3072], P(('row', 'col')), may hold values from 0 to 127
Outputs:
- new_block: float32 [8, 131072], P(None, ('row', 'col'))
- coefficients: float32 [8, 40], replicated
- factor: float32 [8, 8], replicated
The draws below stay inside these ranges and needn't reach their ends.
Inputs may be any that keep to these rules, and one draw needn't show every extreme that they name: `tile_rows`: each device's 96 tiles come in 8 runs of 12; the row tiles of run k are 12 distinct values from k * 32 to (k + 1) * 32 - 1.
All inputs are finite; a program needn't handle non-finite values.
Results may differ from the reference program's by a relative error of at most 0.0054.
Values may be sent and summed in bfloat16 or wider, within the bound.
A program may use at most 64 MiB of HBM per device.

```python
import math
import jax
import jax.numpy as jnp
from jax import lax

LOC = 4096
CAP = 12
TILE = 128
KD = 40
BS = 8
TPD = 96
NTOT = 131072
N_ROW = 4
N_COL = 8


def draw_basis(key, part):
    key_noise, key_common, key_lean = jax.random.split(key, 3)
    random_part = jax.random.normal(key_noise, (KD, NTOT), jnp.float32)
    common = jax.random.normal(key_common, (NTOT,), jnp.float32)
    leaning = jax.random.uniform(key_lean, (KD,), jnp.float32, -0.7, 0.7)
    return (random_part + leaning[:, None] * common[None, :]).astype(jnp.bfloat16)


def draw_tile_rows(key, part):
    region = LOC // TILE
    runs = N_ROW * N_COL * N_COL
    subkeys = jax.random.split(jax.random.fold_in(key, 7), runs)
    chosen = jax.vmap(lambda subkey: jax.random.permutation(subkey, region))(subkeys)[:, :CAP]
    offsets = jnp.arange(runs, dtype=jnp.int32) % N_COL * region
    return (chosen.astype(jnp.int32) + offsets[:, None]).reshape(runs * CAP).astype(jnp.int32)


def with_ends(array, stream_key, smallest, high):
    extent = array.shape
    place = [jax.random.randint(jax.random.fold_in(stream_key, axis), (), 0, extent[axis]) for axis in range(len(extent))]
    array = array.at[tuple(place)].set(smallest)
    longest = extent.index(max(extent))
    place[longest] = (place[longest] + 1) % extent[longest]
    return array.at[tuple(place)].set(high)


def block_scale(key, extent, shards, least, high):
    def one(dim, blocks):
        heights = jax.random.uniform(jax.random.fold_in(jax.random.fold_in(key, 6), dim), (blocks,), jnp.float32, least / len(shards), high / len(shards))
        return jnp.repeat(jnp.exp(heights), extent[dim] // blocks).reshape((-1,) + (1,) * (len(extent) - dim - 1))

    factor_of = one(*shards[0])
    for cut in shards[1:]:
        factor_of = factor_of * one(*cut)
    return factor_of


def noise(key, shape, scale, reach, pieces=(), kind=jnp.bfloat16):
    values = jax.random.normal(key, shape, jnp.float32) * scale
    if len(pieces) > 0:
        values = block_scale(key, shape, pieces, -0.22, 0.18) * values
    return jnp.clip(values, min=-reach, max=reach).astype(kind)


def setup_inputs(seed: int = 0) -> dict:
    key_of = jax.random.split(jax.random.key(seed), 6)
    return {
        "basis": draw_basis(jax.random.fold_in(key_of[5], 71), 0),
        "expand": noise(key_of[1], (3, BS, KD), KD ** -0.5, 1.0, (), jnp.float32),
        "tiles": noise(key_of[2], (3, TPD * N_ROW * N_COL, TILE, TILE), (TPD * TILE * TILE // LOC) ** -0.5, 0.3125, ((1, 32),)),
        "tile_rows": draw_tile_rows(jax.random.fold_in(key_of[5], 71), 0),
        "tile_cols": with_ends(jax.random.randint(key_of[4], (TPD * N_ROW * N_COL,), 0, N_ROW * LOC // TILE), jax.random.fold_in(key_of[4], 1), 0, (N_ROW * LOC // TILE) - 1).astype(jnp.int32),
    }


def reference(basis, expand, tiles, tile_rows, tile_cols):
    entries = LOC * N_ROW * N_COL
    inverse_root = 1.0 / math.sqrt(entries)
    highest = lax.Precision.HIGHEST
    basis_full = basis.astype(jnp.float32)
    series = jnp.einsum('mbk,kn->mbn', expand.astype(jnp.float32), basis_full, precision=highest).astype(jnp.bfloat16)
    layout = series.reshape(3, BS, N_ROW, N_COL, LOC)
    region = LOC // TILE
    slot_count = N_COL * region

    def device(index_dev, sums_row):
        index_dev = index_dev.astype(jnp.int32)
        row_index = index_dev // N_COL
        col_index = index_dev % N_COL
        columns = lax.dynamic_index_in_dim(layout, col_index, 3, keepdims=False)
        columns = columns.reshape(3, BS, N_ROW * LOC // TILE, TILE)
        start = (index_dev * TPD).astype(jnp.int32)
        matrices = lax.dynamic_slice_in_dim(tiles, start, TPD, 1).astype(jnp.float32)
        rows_here = lax.dynamic_slice_in_dim(tile_rows, start, TPD, 0)
        cols_here = lax.dynamic_slice_in_dim(tile_cols, start, TPD, 0)
        picked = jnp.take(columns, cols_here, axis=2).astype(jnp.float32)
        products = jnp.einsum('mtij,mbtj->bti', matrices, picked, precision=highest)
        onehot = (rows_here[:, None] == jnp.arange(slot_count, dtype=jnp.int32)[None, :]).astype(jnp.float32)
        partial_value = jnp.einsum('ts,bti->bsi', onehot, products, precision=highest).reshape(BS, slot_count * TILE)
        return sums_row.at[:, row_index].add(partial_value)
    sums_row = lax.fori_loop(0, N_ROW * N_COL, device, jnp.zeros((BS, N_ROW, slot_count * TILE), jnp.float32))
    applied = sums_row.reshape(BS, entries)
    first_pass = jnp.dot(applied, basis_full.T, precision=highest) * inverse_root
    projected = applied - jnp.dot(first_pass, basis_full, precision=highest) * inverse_root
    second_pass = jnp.dot(projected, basis_full.T, precision=highest) * inverse_root
    cleaned = projected - jnp.dot(second_pass, basis_full, precision=highest) * inverse_root
    coefficients = first_pass + second_pass
    gram_block = jnp.dot(cleaned, cleaned.T, precision=highest) / entries
    factor = jnp.linalg.cholesky(gram_block)
    new_block = lax.linalg.triangular_solve(factor, cleaned, left_side=True, lower=True)
    return (new_block, coefficients, factor)
```

```python
import functools
import math

import jax
import jax.numpy as jnp
from jax import lax
from jax.experimental import pallas as pl
from jax.experimental.pallas import tpu as pltpu
from jax.sharding import PartitionSpec as P

F32 = jnp.float32
BF16 = jnp.bfloat16
NT = (((1,), (1,)), ((), ()))


def exact(a, b, dims=(((1,), (0,)), ((), ()))):
    return lax.dot_general(a, b, dims, precision=lax.Precision.HIGHEST, preferred_element_type=F32)


def pieces(x):
    one = x.astype(BF16).astype(F32)
    rest = x - one
    two = rest.astype(BF16).astype(F32)
    three = rest - two
    return jnp.concatenate([one, two, three], axis=0).astype(BF16)


def fold(x, rows):
    return x[:rows] + x[rows : 2 * rows] + x[2 * rows :]


def kernel(
    nrow,
    ncol,
    expand_hbm,
    rows_hbm,
    picks_hbm,
    basis_hbm,
    tiles_hbm,
    new_ref,
    coef_ref,
    factor_ref,
    expand_ref,
    rows_ref,
    picks_ref,
    basis,
    tiles,
    cols,
    outbox,
    inbox,
    seg_out,
    seg_in,
    corr_col,
    corr_row,
    tail_col,
    tail_row,
    spread,
    app,
    small_sem,
    basis_sem,
    tile_sem,
    ser_send,
    ser_recv,
    fwd_recv,
    seg_send,
    seg_recv,
    box_send,
    box_recv,
    cc_send,
    cc_recv,
    cr_send,
    cr_recv,
    tc_send,
    tc_recv,
    tr_send,
    tr_recv,
):
    r = lax.axis_index("row")
    c = lax.axis_index("col")
    krylov, length = basis.shape
    kinds, tpd, tile, _ = tiles.shape
    cap = tpd // ncol
    region = length // tile
    bs = expand_ref.shape[1]
    entries = length * nrow * ncol
    inverse_root = 1.0 / math.sqrt(entries)
    width = seg_in.shape[2]

    load_basis = pltpu.make_async_copy(basis_hbm, basis, basis_sem)
    load_basis.start()
    small = [
        pltpu.make_async_copy(src, dst, small_sem.at[i])
        for i, (src, dst) in enumerate(((expand_hbm, expand_ref), (rows_hbm, rows_ref), (picks_hbm, picks_ref)))
    ]
    for copy in small:
        copy.start()

    barrier = pltpu.get_barrier_semaphore()
    for j in range(1, nrow):
        pl.semaphore_signal(barrier, inc=1, device_id={"row": lax.rem(r + j, nrow)}, device_id_type=pl.DeviceIdType.MESH)
    for j in range(1, ncol):
        pl.semaphore_signal(barrier, inc=1, device_id={"col": lax.rem(c + j, ncol)}, device_id_type=pl.DeviceIdType.MESH)

    def remote(src, dst, send_sem, recv_sem, where):
        return pltpu.make_async_remote_copy(
            src_ref=src, dst_ref=dst, send_sem=send_sem, recv_sem=recv_sem,
            device_id=where, device_id_type=pl.DeviceIdType.MESH,
        )

    def landed(ref, sem):
        part = ref.at[pl.ds(0, ref.shape[0] - 1)]
        pltpu.make_async_copy(part, part, sem).wait()

    def row_at(j):
        peer = lax.rem(r + j, nrow)
        return peer, {"row": peer}

    def col_at(j):
        peer = lax.rem(c + j, ncol)
        return peer, {"col": peer}

    small[0].wait()
    load_basis.wait()
    for m in range(kinds):
        for k in range(ncol):
            part = pl.ds(k * cap, cap)
            pltpu.make_async_copy(tiles_hbm.at[m, part], tiles.at[m, part], tile_sem.at[m]).start()

    expand = pieces(expand_ref[...].reshape(kinds * bs, krylov))
    for l in range(region):
        part = fold(jnp.dot(expand, basis[:, l * tile : (l + 1) * tile], preferred_element_type=F32), kinds * bs)
        for m in range(kinds):
            cols[m, r * region + l] = part[m * bs : (m + 1) * bs].astype(BF16)

    pl.semaphore_wait(barrier, nrow + ncol - 2)

    outer = nrow // 2
    side, pair = lax.rem(r, 2), lax.div(r, 2)
    mate = r + 1 - 2 * side
    half = region // 2

    def other(j):
        return 2 * lax.rem(pair + j, outer) + side

    def series_copy(m, owner, peer, slot):
        block = cols.at[m, pl.ds(owner * region, region)]
        return remote(block, block, ser_send, ser_recv.at[m, slot], {"row": peer})

    def pass_on(m, owner, h, peer, slot):
        block = cols.at[m, pl.ds(owner * region + h * half, half)]
        return remote(block, block, ser_send, fwd_recv.at[m, h, slot - 1], {"row": peer})

    for m in range(kinds):
        series_copy(m, r, mate, 0).start()
        for j in range(1, outer):
            series_copy(m, r, other(j), outer - j).start()

    small[1].wait()
    small[2].wait()

    slot = lax.broadcasted_iota(jnp.int32, (1, width), 1)
    for k in range(ncol):
        line = jnp.zeros((1, width), jnp.int32)
        for t in range(cap):
            line = jnp.where(lax.rem(slot, cap) == t, rows_ref[k * cap + t], line)
        seg_out[k] = line
    for j in range(1, ncol):
        peer, where = col_at(j)
        remote(seg_out.at[peer], seg_in.at[c], seg_send, seg_recv, where).start()
    seg_in[c] = seg_out[c]

    corr = lax.dot_general(basis[...], basis[...], NT, preferred_element_type=F32)
    band = corr_col.shape[1]
    lanes = corr_col.shape[2]
    folds = -(-krylov // band)
    corr = jnp.pad(corr, ((0, folds * band - krylov), (0, 0)))
    corr_col[c] = jnp.concatenate(
        [corr[i * band : (i + 1) * band] for i in range(folds)] + [jnp.zeros((band, lanes - folds * krylov), F32)], axis=1
    )
    for j in range(1, ncol):
        peer, where = col_at(j)
        remote(corr_col.at[c], corr_col.at[c], cc_send, cc_recv, where).start()

    def relay(m):
        series_copy(m, mate, mate, 0).wait_recv()
        for j in range(1, outer):
            pass_on(m, mate, 1, other(j), outer - j).start()
        for j in range(1, outer):
            series_copy(m, other(j), other(j), j).wait_recv()
            pass_on(m, other(j), 0, mate, j).start()

    def relayed(m):
        for j in range(1, outer):
            far = other(j) + 1 - 2 * side
            pass_on(m, far, 0, mate, j).wait_recv()
            pass_on(m, far, 1, mate, j).wait_recv()

    for m in range(kinds):
        relay(m)
    landed(corr_col, cc_recv)
    corr_row[r] = jnp.sum(corr_col[...], axis=0)
    for j in range(1, nrow):
        peer, where = row_at(j)
        remote(corr_row.at[r], corr_row.at[r], cr_send, cr_recv, where).start()
    for m in range(kinds):
        relayed(m)

    def products(k, dst):
        for t in range(cap):
            g = k * cap + t
            at = picks_ref[g]
            x = jnp.concatenate([cols[m, at] for m in range(kinds)], axis=1)
            w = jnp.concatenate([tiles[m, g] for m in range(kinds)], axis=1)
            dst[k, t] = lax.dot_general(x, w, NT, preferred_element_type=F32).astype(BF16)

    def box_copy(k, where):
        return remote(outbox.at[k], inbox.at[c], box_send, box_recv, where)

    def chunk(j, carry):
        k, where = col_at(j)
        products(k, outbox)
        box_copy(k, where).start()
        return carry

    for m in range(kinds):
        pltpu.make_async_copy(tiles_hbm.at[m], tiles.at[m], tile_sem.at[m]).wait()
    lax.fori_loop(1, ncol, chunk, 0)
    products(c, inbox)

    landed(seg_in, seg_recv)
    line = seg_in[0]
    for k in range(1, ncol):
        line = jnp.where(lax.div(slot, cap) == k, seg_in[k], line)
    here = lax.broadcasted_iota(jnp.int32, (region, tpd), 0) + c * region
    onehot = (line[:, :tpd] == here).astype(F32).astype(BF16)

    landed(corr_row, cr_recv)
    corr = jnp.sum(corr_row[...], axis=0) / entries
    corr = jnp.concatenate([corr[:, i * krylov : (i + 1) * krylov] for i in range(folds)], axis=0)[:krylov]
    eye = (
        lax.broadcasted_iota(jnp.int32, (krylov, krylov), 0) == lax.broadcasted_iota(jnp.int32, (krylov, krylov), 1)
    ).astype(F32)
    once = eye - corr
    both = eye + once
    kern = exact(both, eye + exact(once, once))

    landed(inbox, box_recv)
    spread[...] = inbox[...].astype(F32).reshape(tpd, bs, tile)
    for b in range(bs):
        app[:, b, :] = jnp.dot(onehot, spread[:, b, :].astype(BF16), preferred_element_type=F32)
    applied = jnp.concatenate([app[s] for s in range(region)], axis=1)

    split = pieces(applied)
    raw = fold(lax.dot_general(split, basis[...], NT, preferred_element_type=F32), bs)
    energy = fold(lax.dot_general(split, split, NT, preferred_element_type=F32), bs)
    energy = energy[:, :bs] + energy[:, bs : 2 * bs] + energy[:, 2 * bs :]
    tail_col[c] = jnp.concatenate([raw, energy, jnp.zeros((bs, 128 - krylov - bs), F32)], axis=1)
    for j in range(1, ncol):
        peer, where = col_at(j)
        remote(tail_col.at[c], tail_col.at[c], tc_send, tc_recv, where).start()
    landed(tail_col, tc_recv)
    tail_row[r] = jnp.sum(tail_col[...], axis=0)
    for j in range(1, nrow):
        peer, where = row_at(j)
        remote(tail_row.at[r], tail_row.at[r], tr_send, tr_recv, where).start()
    landed(tail_row, tr_recv)
    total = jnp.sum(tail_row[...], axis=0)

    first = total[:, :krylov] * inverse_root
    coefficients = exact(first, both)
    gram = (total[:, krylov : krylov + bs] - exact(exact(first, kern), first, NT)) / entries
    coef_ref[...] = coefficients

    sub = lax.broadcasted_iota(jnp.int32, (bs, bs), 0)
    lane = lax.broadcasted_iota(jnp.int32, (bs, bs), 1)
    up = lax.broadcasted_iota(jnp.int32, (bs, 1), 0)
    factor = jnp.zeros((bs, bs), F32)
    inverse = jnp.zeros((bs, 1), F32)
    steps = []
    for j in range(bs):
        column, line = gram[:, j : j + 1], gram[j : j + 1, :]
        pivot = jnp.sqrt(gram[j : j + 1, j : j + 1])
        column = jnp.where(up >= j, column / pivot, 0.0)
        factor = jnp.where(lane == j, column, factor)
        inverse = jnp.where(up == j, 1.0 / pivot, inverse)
        steps.append(jnp.where(up > j, column, 0.0))
        gram = gram - column * (line / pivot)
    factor_ref[...] = factor

    cleaned = applied - fold(
        jnp.dot(pieces(coefficients * inverse_root), basis[...], preferred_element_type=F32), bs
    )
    solved = cleaned * inverse
    for j in range(bs - 1):
        solved = solved - (steps[j] * inverse) * solved[j : j + 1, :]
    new_ref[...] = solved

    sent = cols.at[:, pl.ds(0, (nrow - 1) * region)]
    pltpu.make_async_copy(sent, sent, ser_send).wait()
    for ref, sem in (
        (seg_in, seg_send), (corr_col, cc_send), (inbox, box_send), (tail_col, tc_send), (corr_row, cr_send), (tail_row, tr_send)
    ):
        landed(ref, sem)


def leave(new_ref, coef_ref, factor_ref, new_hbm, coef_hbm, factor_hbm, sem):
    copies = [
        pltpu.make_async_copy(src, dst, sem.at[i])
        for i, (src, dst) in enumerate(((new_ref, new_hbm), (coef_ref, coef_hbm), (factor_ref, factor_hbm)))
    ]
    for copy in copies:
        copy.start()
    for copy in copies:
        copy.wait()


def shards(basis, expand, tiles, tile_rows, tile_cols):
    nrow = lax.axis_size("row")
    ncol = lax.axis_size("col")
    krylov, length = basis.shape
    kinds, tpd, tile, _ = tiles.shape
    bs = expand.shape[1]
    region = length // tile
    cap = tpd // ncol
    width = -(-tpd // 128) * 128
    dma = pltpu.SemaphoreType.DMA
    band = 16
    lanes = -(-(-(-krylov // band) * krylov) // 128) * 128
    vmem, hbm = pl.BlockSpec(memory_space=pltpu.VMEM), pl.BlockSpec(memory_space=pltpu.HBM)
    shapes = (
        jax.ShapeDtypeStruct((bs, length), F32),
        jax.ShapeDtypeStruct((bs, krylov), F32),
        jax.ShapeDtypeStruct((bs, bs), F32),
    )
    held = pl.pallas_call(
        functools.partial(kernel, nrow, ncol),
        out_shape=shapes,
        in_specs=[hbm] * 5,
        out_specs=(vmem, vmem, vmem),
        scratch_shapes=[
            pltpu.VMEM(expand.shape, F32),
            pltpu.SMEM((tpd,), jnp.int32),
            pltpu.SMEM((tpd,), jnp.int32),
            pltpu.VMEM((krylov, length), BF16),
            pltpu.VMEM((kinds, tpd, tile, tile), BF16),
            pltpu.VMEM((kinds, nrow * region, bs, tile), BF16),
            pltpu.VMEM((ncol, cap, bs, tile), BF16),
            pltpu.VMEM((ncol, cap, bs, tile), BF16),
            pltpu.VMEM((ncol, 1, width), jnp.int32),
            pltpu.VMEM((ncol, 1, width), jnp.int32),
            pltpu.VMEM((ncol, band, lanes), F32),
            pltpu.VMEM((nrow, band, lanes), F32),
            pltpu.VMEM((ncol, bs, 128), F32),
            pltpu.VMEM((nrow, bs, 128), F32),
            pltpu.VMEM((tpd, bs, tile), F32),
            pltpu.VMEM((region, bs, tile), F32),
            dma((3,)),
            dma,
            dma((kinds,)),
            dma,
            dma((kinds, nrow // 2)),
            dma((kinds, 2, nrow // 2 - 1)),
        ]
        + [dma] * 12,
        compiler_params=pltpu.CompilerParams(
            collective_id=0, has_side_effects=True, vmem_limit_bytes=48 * 1024 * 1024
        ),
    )(*(pltpu.with_memory_space_constraint(x, pltpu.HBM) for x in (expand, tile_rows, tile_cols, basis, tiles)))
    return pl.pallas_call(
        leave,
        out_shape=shapes,
        in_specs=[vmem] * 3,
        out_specs=(hbm, hbm, hbm),
        scratch_shapes=[dma((3,))],
    )(*(pltpu.with_memory_space_constraint(x, pltpu.VMEM) for x in held))


def solution(mesh):
    return jax.shard_map(
        shards,
        mesh=mesh,
        in_specs=(
            P(None, ("row", "col")),
            P(),
            P(None, ("row", "col"), None, None),
            P(("row", "col")),
            P(("row", "col")),
        ),
        out_specs=(P(None, ("row", "col")), P(), P()),
        check_vma=False,
    )
```

```python
import functools
import math

import jax
import jax.numpy as jnp
from jax import lax
from jax.experimental import pallas as pl
from jax.experimental.pallas import tpu as pltpu
from jax.sharding import PartitionSpec as P

F32 = jnp.float32
BF16 = jnp.bfloat16
NT = (((1,), (1,)), ((), ()))


def exact(a, b, dims=(((1,), (0,)), ((), ()))):
    return lax.dot_general(a, b, dims, precision=lax.Precision.HIGHEST, preferred_element_type=F32)


def pieces(x):
    one = x.astype(BF16).astype(F32)
    return jnp.concatenate([one, x - one], axis=0).astype(BF16)


def fold(x, rows):
    return x[:rows] + x[rows:]


def kernel(
    nrow,
    ncol,
    expand_hbm,
    rows_hbm,
    picks_hbm,
    basis_hbm,
    tiles_hbm,
    new_ref,
    coef_ref,
    factor_ref,
    expand_ref,
    rows_ref,
    picks_ref,
    basis,
    tiles,
    cols,
    outbox,
    inbox,
    seg_out,
    seg_in,
    corr_col,
    corr_row,
    tail,
    place,
    small_sem,
    basis_sem,
    tile_sem,
    ser_send,
    ser_recv,
    fwd_recv,
    seg_send,
    seg_recv,
    box_send,
    box_recv,
    cc_send,
    cc_recv,
    cr_send,
    cr_recv,
    tail_send,
    tail_recv,
    low_sem,
    high_sem,
):
    r = lax.axis_index("row")
    c = lax.axis_index("col")
    krylov, length = basis.shape
    kinds, tpd, tile, _ = tiles.shape
    cap = tpd // ncol
    region = length // tile
    bs = expand_ref.shape[1]
    entries = length * nrow * ncol
    inverse_root = 1.0 / math.sqrt(entries)
    width = seg_in.shape[2]

    load_basis = pltpu.make_async_copy(basis_hbm, basis, basis_sem)
    load_basis.start()
    small = [
        pltpu.make_async_copy(src, dst, small_sem.at[i])
        for i, (src, dst) in enumerate(((expand_hbm, expand_ref), (rows_hbm, rows_ref), (picks_hbm, picks_ref)))
    ]
    for copy in small:
        copy.start()

    outer = nrow // 2
    side, pair = lax.rem(r, 2), lax.div(r, 2)
    mate = r + 1 - 2 * side
    half = region // 2

    def other(j):
        return 2 * lax.rem(pair + j, outer) + side

    def signal(sem, where):
        pl.semaphore_signal(sem, inc=1, device_id=where, device_id_type=pl.DeviceIdType.MESH)

    barrier = pltpu.get_barrier_semaphore()
    has_low, has_high = c >= 2, c < ncol - 2
    even = c - lax.rem(c, 2)

    def low(i):
        return {"col": lax.rem(even - 2 + i + ncol, ncol)}

    def high(i):
        return {"col": lax.rem(even + 2 + i, ncol)}

    signal(barrier, {"row": mate})
    for j in range(1, outer):
        signal(barrier, {"row": other(j)})
    signal(barrier, {"col": c + 1 - 2 * lax.rem(c, 2)})
    for i in range(2):
        pl.when(has_low)(lambda: signal(barrier, low(i)))
        pl.when(has_high)(lambda: signal(barrier, high(i)))

    def tell(i):
        pl.when(has_low)(lambda: signal(high_sem.at[i], low(lax.rem(c, 2))))
        pl.when(has_high)(lambda: signal(low_sem.at[i], high(lax.rem(c, 2))))

    def hear(i):
        pl.when(has_low)(lambda: pl.semaphore_wait(low_sem.at[i], 1))
        pl.when(has_high)(lambda: pl.semaphore_wait(high_sem.at[i], 1))

    def remote(src, dst, send_sem, recv_sem, where):
        return pltpu.make_async_remote_copy(
            src_ref=src, dst_ref=dst, send_sem=send_sem, recv_sem=recv_sem,
            device_id=where, device_id_type=pl.DeviceIdType.MESH,
        )

    def landed(ref, sem):
        part = ref.at[pl.ds(0, ref.shape[0] - 1)]
        pltpu.make_async_copy(part, part, sem).wait()

    def row_at(j):
        peer = lax.rem(r + j, nrow)
        return peer, {"row": peer}

    def col_at(j):
        peer = lax.rem(c + j, ncol)
        return peer, {"col": peer}

    small[0].wait()
    load_basis.wait()
    for m in range(kinds):
        for k in range(ncol):
            part = pl.ds(k * cap, cap)
            pltpu.make_async_copy(tiles_hbm.at[m, part], tiles.at[m, part], tile_sem.at[m]).start()

    expand = pieces(expand_ref[...].reshape(kinds * bs, krylov))
    for l in range(region):
        part = fold(jnp.dot(expand, basis[:, l * tile : (l + 1) * tile], preferred_element_type=F32), kinds * bs)
        for m in range(kinds):
            cols[m, r * region + l] = part[m * bs : (m + 1) * bs].astype(BF16)

    pl.semaphore_wait(barrier, outer + 1 + 2 * (has_low.astype(jnp.int32) + has_high.astype(jnp.int32)))

    def series_copy(m, owner, peer, slot):
        block = cols.at[m, pl.ds(owner * region, region)]
        return remote(block, block, ser_send, ser_recv.at[m, slot], {"row": peer})

    def pass_on(m, owner, h, peer, slot):
        block = cols.at[m, pl.ds(owner * region + h * half, half)]
        return remote(block, block, ser_send, fwd_recv.at[m, h, slot - 1], {"row": peer})

    for m in range(kinds):
        series_copy(m, r, mate, 0).start()
        for j in range(1, outer):
            series_copy(m, r, other(j), outer - j).start()

    rounds = ncol // 2 - 2
    if rounds > 0:
        tell(0)

    small[1].wait()
    small[2].wait()
    slot = lax.broadcasted_iota(jnp.int32, (1, width), 1)
    entry, inner = lax.rem(lax.div(slot, bs), cap), lax.rem(slot, bs)
    for k in range(ncol):
        line = jnp.zeros((1, width), jnp.int32)
        for t in range(cap):
            line = jnp.where(entry == t, rows_ref[k * cap + t] * bs, line)
        seg_out[k] = line + inner
    seg_in[c] = seg_out[c]

    corr = lax.dot_general(basis[...], basis[...], NT, preferred_element_type=F32)
    band = corr_col.shape[1]
    lanes = corr_col.shape[2]
    folds = -(-krylov // band)
    corr = jnp.pad(corr, ((0, folds * band - krylov), (0, 0)))
    corr_col[c] = jnp.concatenate(
        [corr[i * band : (i + 1) * band] for i in range(folds)] + [jnp.zeros((band, lanes - folds * krylov), F32)], axis=1
    )

    def relay(m):
        series_copy(m, mate, mate, 0).wait_recv()
        for j in range(1, outer):
            pass_on(m, mate, 1, other(j), outer - j).start()
        for j in range(1, outer):
            series_copy(m, other(j), other(j), j).wait_recv()
            pass_on(m, other(j), 0, mate, j).start()

    def relayed(m):
        for j in range(1, outer):
            far = other(j) + 1 - 2 * side
            pass_on(m, far, 0, mate, j).wait_recv()
            pass_on(m, far, 1, mate, j).wait_recv()

    relay(0)
    for i in range(rounds - 1):
        hear(i)
        tell(i + 1)
    relay(1)
    if rounds > 0:
        hear(rounds - 1)
    for j in range(1, ncol):
        peer, where = col_at(j)
        remote(seg_out.at[peer], seg_in.at[c], seg_send, seg_recv, where).start()
    for j in range(1, ncol):
        peer, where = col_at(j)
        remote(corr_col.at[c], corr_col.at[c], cc_send, cc_recv, where).start()
    for m in range(2, kinds):
        relay(m)
    for m in range(kinds):
        relayed(m)

    def products(k, dst):
        for t in range(0, cap, 2):
            both = []
            for g in (k * cap + t, k * cap + t + 1):
                at = picks_ref[g]
                x = jnp.concatenate([cols[m, at] for m in range(kinds)], axis=1)
                w = jnp.concatenate([tiles[m, g] for m in range(kinds)], axis=1)
                both.append(lax.dot_general(x, w, NT, preferred_element_type=F32))
            dst[k, t * bs : (t + 2) * bs] = jnp.concatenate(both, axis=0).astype(BF16)

    def box_copy(k, where):
        return remote(outbox.at[k], inbox.at[c], box_send, box_recv, where)

    def chunk(j, carry):
        k, where = col_at(j)
        products(k, outbox)
        box_copy(k, where).start()
        return carry

    for m in range(kinds):
        pltpu.make_async_copy(tiles_hbm.at[m], tiles.at[m], tile_sem.at[m]).wait()
    lax.fori_loop(1, ncol, chunk, 0)
    products(c, inbox)

    landed(corr_col, cc_recv)
    corr_row[r] = jnp.sum(corr_col[...], axis=0)
    for j in range(1, nrow):
        peer, where = row_at(j)
        remote(corr_row.at[r], corr_row.at[r], cr_send, cr_recv, where).start()
    landed(seg_in, seg_recv)
    line = seg_in[0]
    for k in range(1, ncol):
        line = jnp.where(lax.div(slot, cap * bs) == k, seg_in[k], line)
    here = lax.broadcasted_iota(jnp.int32, (region * bs, tpd * bs), 0) + c * (region * bs)
    place[...] = (line[:, : tpd * bs] == here).astype(F32).astype(BF16)

    landed(inbox, box_recv)
    app = jnp.dot(place[...], inbox[...].reshape(tpd * bs, tile), preferred_element_type=F32)
    applied = jnp.concatenate([app[s * bs : (s + 1) * bs] for s in range(region)], axis=1)

    split = pieces(applied)
    stack = jnp.concatenate([split, basis[...]], axis=0)
    raw = fold(lax.dot_general(split, stack, NT, preferred_element_type=F32), bs)
    raw = jnp.concatenate([raw, jnp.zeros((bs, 64 - 2 * bs - krylov), F32)], axis=1)
    me = r * ncol + c
    tail[me] = jnp.concatenate([raw[: bs // 2], raw[bs // 2 :]], axis=1)

    for j in sorted(range(ncol), key=lambda j: -min(j, ncol - j)):
        for i in reversed(range(nrow)):
            if i or j:
                where = {"row": lax.rem(r + i, nrow), "col": lax.rem(c + j, ncol)}
                remote(tail.at[me], tail.at[me], tail_send, tail_recv, where).start()

    landed(corr_row, cr_recv)
    corr = jnp.sum(corr_row[...], axis=0) / entries
    corr = jnp.concatenate([corr[:, i * krylov : (i + 1) * krylov] for i in range(folds)], axis=0)[:krylov]
    eye = (
        lax.broadcasted_iota(jnp.int32, (krylov, krylov), 0) == lax.broadcasted_iota(jnp.int32, (krylov, krylov), 1)
    ).astype(F32)
    once = eye - corr
    both = eye + once
    kern = exact(both, eye + exact(once, once)) * (inverse_root / entries * inverse_root)
    before, after = 2 * bs, 64 - 2 * bs - krylov
    both = jnp.pad(both * inverse_root, ((before, after), (0, 0)))
    kern = jnp.pad(kern, ((before, after), (before, after)))
    down, along = (lax.broadcasted_iota(jnp.int32, (64, bs), d) for d in (0, 1))
    gather = ((down == along) | (down == along + bs)).astype(F32)

    landed(tail, tail_recv)

    total = jnp.sum(tail[...], axis=0)
    total = jnp.concatenate([total[:, :64], total[:, 64:]], axis=0)
    gram = exact(total, gather) / entries - exact(exact(total, kern), total, NT)
    coefficients = exact(total, both)
    coef_ref[...] = coefficients

    sub = lax.broadcasted_iota(jnp.int32, (bs, tile), 0)
    lane = lax.broadcasted_iota(jnp.int32, (bs, tile), 1)
    columns = [jnp.broadcast_to(gram[:, j : j + 1], (bs, tile)) for j in range(bs)]
    factor = jnp.zeros((bs, tile), F32)
    inverse = jnp.zeros((bs, tile), F32)
    for j in range(bs):
        root = jnp.broadcast_to(lax.rsqrt(columns[j][j : j + 1]), (bs, tile))
        column = jnp.where(sub >= j, columns[j] * root, 0.0)
        for k in range(j + 1, bs):
            columns[k] = columns[k] - column * column[k : k + 1]
        factor = jnp.where(lane == j, column, factor)
        inverse = jnp.where(sub == j, root, inverse)
        columns[j] = jnp.where(sub > j, column, 0.0)
    factor_ref[...] = factor[:, :bs]

    correction = fold(jnp.dot(pieces(coefficients * inverse_root), basis[...], preferred_element_type=F32), bs)
    steps = [columns[j] * inverse for j in range(bs - 1)]
    for s in range(region):
        part = slice(s * tile, (s + 1) * tile)
        solved = (applied[:, part] - correction[:, part]) * inverse
        for j in range(bs - 1):
            solved = solved - steps[j] * solved[j : j + 1]
        new_ref[:, part] = solved

    sent = cols.at[:, pl.ds(0, (nrow - 1) * region)]
    pltpu.make_async_copy(sent, sent, ser_send).wait()
    for ref, sem in (
        (seg_in, seg_send), (corr_col, cc_send), (inbox, box_send), (corr_row, cr_send), (tail, tail_send)
    ):
        landed(ref, sem)


def leave(new_ref, coef_ref, factor_ref, new_hbm, coef_hbm, factor_hbm, sem):
    copies = [
        pltpu.make_async_copy(src, dst, sem.at[i])
        for i, (src, dst) in enumerate(((new_ref, new_hbm), (coef_ref, coef_hbm), (factor_ref, factor_hbm)))
    ]
    for copy in copies:
        copy.start()
    for copy in copies:
        copy.wait()


def shards(basis, expand, tiles, tile_rows, tile_cols):
    nrow = lax.axis_size("row")
    ncol = lax.axis_size("col")
    krylov, length = basis.shape
    kinds, tpd, tile, _ = tiles.shape
    bs = expand.shape[1]
    region = length // tile
    cap = tpd // ncol
    width = -(-tpd * bs // 128) * 128
    dma = pltpu.SemaphoreType.DMA
    band = 16
    lanes = -(-(-(-krylov // band) * krylov) // 128) * 128
    vmem, hbm = pl.BlockSpec(memory_space=pltpu.VMEM), pl.BlockSpec(memory_space=pltpu.HBM)
    shapes = (
        jax.ShapeDtypeStruct((bs, length), F32),
        jax.ShapeDtypeStruct((bs, krylov), F32),
        jax.ShapeDtypeStruct((bs, bs), F32),
    )
    held = pl.pallas_call(
        functools.partial(kernel, nrow, ncol),
        out_shape=shapes,
        in_specs=[hbm] * 5,
        out_specs=(vmem, vmem, vmem),
        scratch_shapes=[
            pltpu.VMEM(expand.shape, F32),
            pltpu.SMEM((tpd,), jnp.int32),
            pltpu.SMEM((tpd,), jnp.int32),
            pltpu.VMEM((krylov, length), BF16),
            pltpu.VMEM((kinds, tpd, tile, tile), BF16),
            pltpu.VMEM((kinds, nrow * region, bs, tile), BF16),
            pltpu.VMEM((ncol, cap * bs, tile), BF16),
            pltpu.VMEM((ncol, cap * bs, tile), BF16),
            pltpu.VMEM((ncol, 1, width), jnp.int32),
            pltpu.VMEM((ncol, 1, width), jnp.int32),
            pltpu.VMEM((ncol, band, lanes), F32),
            pltpu.VMEM((nrow, band, lanes), F32),
            pltpu.VMEM((nrow * ncol, bs // 2, 128), F32),
            pltpu.VMEM((region * bs, tpd * bs), BF16),
            dma((3,)),
            dma,
            dma((kinds,)),
            dma,
            dma((kinds, nrow // 2)),
            dma((kinds, 2, nrow // 2 - 1)),
        ]
        + [dma] * 10
        + [pltpu.SemaphoreType.REGULAR((max(ncol // 2 - 2, 1),))] * 2,
        compiler_params=pltpu.CompilerParams(
            collective_id=0, has_side_effects=True, vmem_limit_bytes=48 * 1024 * 1024
        ),
    )(*(pltpu.with_memory_space_constraint(x, pltpu.HBM) for x in (expand, tile_rows, tile_cols, basis, tiles)))
    return pl.pallas_call(
        leave,
        out_shape=shapes,
        in_specs=[vmem] * 3,
        out_specs=(hbm, hbm, hbm),
        scratch_shapes=[dma((3,))],
    )(*(pltpu.with_memory_space_constraint(x, pltpu.VMEM) for x in held))


def solution(mesh):
    return jax.shard_map(
        shards,
        mesh=mesh,
        in_specs=(
            P(None, ("row", "col")),
            P(),
            P(None, ("row", "col"), None, None),
            P(("row", "col")),
            P(("row", "col")),
        ),
        out_specs=(P(None, ("row", "col")), P(), P()),
        check_vma=False,
    )
```

```python
import functools
import math

import jax
import jax.numpy as jnp
from jax import lax
from jax.experimental import pallas as pl
from jax.experimental.pallas import tpu as pltpu
from jax.sharding import PartitionSpec as P

F32 = jnp.float32
BF16 = jnp.bfloat16
NT = (((1,), (1,)), ((), ()))


def exact(a, b, dims=(((1,), (0,)), ((), ()))):
    return lax.dot_general(a, b, dims, precision=lax.Precision.HIGHEST, preferred_element_type=F32)


def pieces(x):
    one = x.astype(BF16).astype(F32)
    return jnp.concatenate([one, x - one], axis=0).astype(BF16)


def fold(x, rows):
    return x[:rows] + x[rows:]


def kernel(
    nrow,
    ncol,
    expand_hbm,
    rows_hbm,
    picks_hbm,
    basis_hbm,
    tiles_hbm,
    new_ref,
    coef_ref,
    factor_ref,
    expand_ref,
    rows_ref,
    picks_ref,
    basis,
    tiles,
    cols0,
    cols1,
    cols2,
    outbox,
    inbox,
    seg_out,
    seg_in,
    corr_col,
    corr_row,
    tail,
    place,
    held,
    small_sem,
    basis_sem,
    tile_sem,
    ser_send,
    ser_recv,
    fwd_recv,
    seg_send,
    seg_recv,
    box_send,
    box_recv,
    cc_send,
    cc_recv,
    cr_send,
    cr_recv,
    tail_send,
    tail_recv,
    low_sem,
    high_sem,
):
    r = lax.axis_index("row")
    c = lax.axis_index("col")
    cols = (cols0, cols1, cols2)
    krylov, length = basis.shape
    kinds, tpd, tile, _ = tiles.shape
    cap = tpd // ncol
    region = length // tile
    bs = expand_ref.shape[1]
    entries = length * nrow * ncol
    inverse_root = 1.0 / math.sqrt(entries)
    width = seg_in.shape[2]

    load_basis = pltpu.make_async_copy(basis_hbm, basis, basis_sem)
    load_basis.start()
    small = [
        pltpu.make_async_copy(src, dst, small_sem.at[i])
        for i, (src, dst) in enumerate(((expand_hbm, expand_ref), (rows_hbm, rows_ref), (picks_hbm, picks_ref)))
    ]
    for copy in small:
        copy.start()

    outer = nrow // 2
    side, pair = lax.rem(r, 2), lax.div(r, 2)
    mate = r + 1 - 2 * side
    half = region // 2

    def other(j):
        return 2 * lax.rem(pair + j, outer) + side

    def signal(sem, where):
        pl.semaphore_signal(sem, inc=1, device_id=where, device_id_type=pl.DeviceIdType.MESH)

    barrier = pltpu.get_barrier_semaphore()
    has_low, has_high = c >= 2, c < ncol - 2
    even = c - lax.rem(c, 2)

    def low(i):
        return {"col": lax.rem(even - 2 + i + ncol, ncol)}

    def high(i):
        return {"col": lax.rem(even + 2 + i, ncol)}

    signal(barrier, {"row": mate})
    for j in range(1, outer):
        signal(barrier, {"row": other(j)})
    signal(barrier, {"col": c + 1 - 2 * lax.rem(c, 2)})
    for i in range(2):
        pl.when(has_low)(lambda: signal(barrier, low(i)))
        pl.when(has_high)(lambda: signal(barrier, high(i)))

    def tell(i):
        pl.when(has_low)(lambda: signal(high_sem.at[i], low(lax.rem(c, 2))))
        pl.when(has_high)(lambda: signal(low_sem.at[i], high(lax.rem(c, 2))))

    def hear(i):
        pl.when(has_low)(lambda: pl.semaphore_wait(low_sem.at[i], 1))
        pl.when(has_high)(lambda: pl.semaphore_wait(high_sem.at[i], 1))

    def remote(src, dst, send_sem, recv_sem, where):
        return pltpu.make_async_remote_copy(
            src_ref=src, dst_ref=dst, send_sem=send_sem, recv_sem=recv_sem,
            device_id=where, device_id_type=pl.DeviceIdType.MESH,
        )

    def landed(ref, sem):
        part = ref.at[pl.ds(0, ref.shape[0] - 1)]
        pltpu.make_async_copy(part, part, sem).wait()

    def row_at(j):
        peer = lax.rem(r + j, nrow)
        return peer, {"row": peer}

    def col_at(j):
        peer = lax.rem(c + j, ncol)
        return peer, {"col": peer}

    small[0].wait()
    load_basis.wait()
    for m in range(kinds):
        for k in range(ncol):
            part = pl.ds(k * cap, cap)
            pltpu.make_async_copy(tiles_hbm.at[m, part], tiles.at[m, part], tile_sem.at[m]).start()

    def make(m):
        one = pieces(expand_ref[m])
        for l in range(region):
            part = jnp.dot(one, basis[:, l * tile : (l + 1) * tile], preferred_element_type=F32)
            cols[m][r * region + l] = fold(part, bs).astype(BF16)

    def series_copy(m, owner, peer, slot):
        block = cols[m].at[pl.ds(owner * region, region)]
        return remote(block, block, ser_send.at[m], ser_recv.at[m, slot], {"row": peer})

    def pass_on(m, owner, h, peer, slot):
        block = cols[m].at[pl.ds(owner * region + h * half, half)]
        return remote(block, block, ser_send.at[m], fwd_recv.at[m, h, slot - 1], {"row": peer})

    def spread(m):
        series_copy(m, r, mate, 0).start()
        for j in range(1, outer):
            series_copy(m, r, other(j), outer - j).start()

    make(0)

    pl.semaphore_wait(barrier, outer + 1 + 2 * (has_low.astype(jnp.int32) + has_high.astype(jnp.int32)))
    spread(0)
    rounds = ncol // 2 - 2
    if rounds > 0:
        tell(0)

    for m in range(1, kinds):
        make(m)
        spread(m)

    small[1].wait()
    small[2].wait()
    slot = lax.broadcasted_iota(jnp.int32, (1, width), 1)
    entry, inner = lax.rem(lax.div(slot, bs), cap), lax.rem(slot, bs)
    for k in range(ncol):
        line = jnp.zeros((1, width), jnp.int32)
        for t in range(cap):
            line = jnp.where(entry == t, rows_ref[k * cap + t] * bs, line)
        seg_out[k] = line + inner
    seg_in[c] = seg_out[c]

    corr = lax.dot_general(basis[...], basis[...], NT, preferred_element_type=F32)
    band = corr_col.shape[1]
    lanes = corr_col.shape[2]
    folds = -(-krylov // band)
    corr = jnp.pad(corr, ((0, folds * band - krylov), (0, 0)))
    corr_col[c] = jnp.concatenate(
        [corr[i * band : (i + 1) * band] for i in range(folds)] + [jnp.zeros((band, lanes - folds * krylov), F32)], axis=1
    )

    def relay(m):
        series_copy(m, mate, mate, 0).wait_recv()
        for j in range(1, outer):
            pass_on(m, mate, 1, other(j), outer - j).start()
        for j in range(1, outer):
            series_copy(m, other(j), other(j), j).wait_recv()
            pass_on(m, other(j), 0, mate, j).start()

    def relayed(m):
        for j in range(1, outer):
            far = other(j) + 1 - 2 * side
            pass_on(m, far, 0, mate, j).wait_recv()
            pass_on(m, far, 1, mate, j).wait_recv()

    relay(0)
    for i in range(rounds - 1):
        hear(i)
        tell(i + 1)
    relay(1)
    if rounds > 0:
        hear(rounds - 1)
    for j in range(1, ncol):
        peer, where = col_at(j)
        remote(seg_out.at[peer], seg_in.at[c], seg_send, seg_recv, where).start()
    for j in range(1, ncol):
        peer, where = col_at(j)
        remote(corr_col.at[c], corr_col.at[c], cc_send, cc_recv, where).start()
    for m in range(2, kinds):
        relay(m)
    for m in range(kinds - 1):
        relayed(m)

    for m in range(kinds):
        pltpu.make_async_copy(tiles_hbm.at[m], tiles.at[m], tile_sem.at[m]).wait()

    def products(k, t, ms):
        out = []
        for g in (k * cap + t, k * cap + t + 1):
            at = picks_ref[g]
            x = jnp.concatenate([cols[m][at] for m in ms], axis=1)
            w = jnp.concatenate([tiles[m, g] for m in ms], axis=1)
            out.append(lax.dot_general(x, w, NT, preferred_element_type=F32))
        return jnp.concatenate(out, axis=0)

    def box_copy(k):
        return remote(outbox.at[k], inbox.at[c], box_send, box_recv, {"col": k})

    across = ncol // 2
    mine = lax.div(c, across)

    def far_side(i):
        return (1 - mine) * across + lax.rem(c + i, across)

    def near_side(i):
        return mine * across + lax.rem(c + i, across)

    early = held.shape[0]
    for i in range(early):
        for t in range(0, cap, 2):
            held[i, t * bs : (t + 2) * bs] = products(far_side(i), t, range(kinds - 1))

    relayed(kinds - 1)

    for i in range(early):
        k = far_side(i)
        for t in range(0, cap, 2):
            rows = slice(t * bs, (t + 2) * bs)
            outbox[k, rows] = (held[i, rows] + products(k, t, (kinds - 1,))).astype(BF16)
        box_copy(k).start()

    def whole(k, dst):
        for t in range(0, cap, 2):
            dst[k, t * bs : (t + 2) * bs] = products(k, t, range(kinds)).astype(BF16)

    def send_far(i, carry):
        whole(far_side(i), outbox)
        box_copy(far_side(i)).start()
        return carry

    def send_near(i, carry):
        whole(near_side(i), outbox)
        box_copy(near_side(i)).start()
        return carry

    lax.fori_loop(early, across, send_far, 0)
    lax.fori_loop(1, across, send_near, 0)

    whole(c, inbox)

    landed(corr_col, cc_recv)
    corr_row[r] = jnp.sum(corr_col[...], axis=0)
    for j in range(1, nrow):
        peer, where = row_at(j)
        remote(corr_row.at[r], corr_row.at[r], cr_send, cr_recv, where).start()
    landed(seg_in, seg_recv)
    line = seg_in[0]
    for k in range(1, ncol):
        line = jnp.where(lax.div(slot, cap * bs) == k, seg_in[k], line)
    here = lax.broadcasted_iota(jnp.int32, (region * bs, tpd * bs), 0) + c * (region * bs)
    place[...] = (line[:, : tpd * bs] == here).astype(F32).astype(BF16)

    landed(inbox, box_recv)
    app = jnp.dot(place[...], inbox[...].reshape(tpd * bs, tile), preferred_element_type=F32)
    applied = jnp.concatenate([app[s * bs : (s + 1) * bs] for s in range(region)], axis=1)

    split = pieces(applied)
    stack = jnp.concatenate([split, basis[...]], axis=0)
    raw = fold(lax.dot_general(split, stack, NT, preferred_element_type=F32), bs)
    raw = jnp.concatenate([raw, jnp.zeros((bs, 64 - 2 * bs - krylov), F32)], axis=1)
    me = r * ncol + c
    tail[me] = jnp.concatenate([raw[: bs // 2], raw[bs // 2 :]], axis=1)

    for j in sorted(range(ncol), key=lambda j: -min(j, ncol - j)):
        for i in reversed(range(nrow)):
            if i or j:
                where = {"row": lax.rem(r + i, nrow), "col": lax.rem(c + j, ncol)}
                remote(tail.at[me], tail.at[me], tail_send, tail_recv, where).start()

    landed(corr_row, cr_recv)
    corr = jnp.sum(corr_row[...], axis=0) / entries
    corr = jnp.concatenate([corr[:, i * krylov : (i + 1) * krylov] for i in range(folds)], axis=0)[:krylov]
    eye = (
        lax.broadcasted_iota(jnp.int32, (krylov, krylov), 0) == lax.broadcasted_iota(jnp.int32, (krylov, krylov), 1)
    ).astype(F32)
    once = eye - corr
    both = eye + once
    kern = exact(both, eye + exact(once, once)) * (inverse_root / entries * inverse_root)
    before, after = 2 * bs, 64 - 2 * bs - krylov
    down, along = (lax.broadcasted_iota(jnp.int32, (64, bs), d) for d in (0, 1))
    gather = ((down == along) | (down == along + bs)).astype(F32) / entries
    mix = jnp.concatenate(
        [
            jnp.pad(both * inverse_root, ((before, after), (0, 0))),
            gather,
            jnp.zeros((64, 64 + before - krylov - bs), F32),
            jnp.pad(kern, ((before, after), (0, after))),
        ],
        axis=1,
    )
    mix = jnp.concatenate([mix, jnp.zeros((64, 128), F32)], axis=0)
    coarse = mix.astype(BF16).astype(F32)
    mix = jnp.concatenate([coarse, mix - coarse], axis=1).astype(BF16)
    right = lax.broadcasted_iota(jnp.int32, (bs, 128), 1) >= 64
    below = lax.broadcasted_iota(jnp.int32, (bs, 128), 0) >= bs // 2

    landed(tail, tail_recv)

    total = jnp.sum(tail[...], axis=0)
    turned = jnp.concatenate([total[:, 64:], total[:, :64]], axis=1)
    total = jnp.where(right == below, jnp.concatenate([total, total], axis=0), jnp.concatenate([turned, turned], axis=0))
    total = pieces(total)
    made = fold(jnp.dot(total, mix, preferred_element_type=F32), bs)
    made = made[:, :128] + made[:, 128:]
    taken = pieces(jnp.where(right, made, 0.0))
    taken = fold(lax.dot_general(taken, total, NT, preferred_element_type=F32), bs)
    gram = made[:, krylov : krylov + bs] - (taken[:, :bs] + taken[:, bs:])
    coefficients = made[:, :krylov]
    coef_ref[...] = coefficients

    sub = lax.broadcasted_iota(jnp.int32, (bs, tile), 0)
    lane = lax.broadcasted_iota(jnp.int32, (bs, tile), 1)
    columns = [jnp.broadcast_to(gram[:, j : j + 1], (bs, tile)) for j in range(bs)]
    factor = jnp.zeros((bs, tile), F32)
    inverse = jnp.zeros((bs, tile), F32)
    for j in range(bs):
        root = jnp.broadcast_to(lax.rsqrt(columns[j][j : j + 1]), (bs, tile))
        column = jnp.where(sub >= j, columns[j] * root, 0.0)
        for k in range(j + 1, bs):
            columns[k] = columns[k] - column * column[k : k + 1]
        factor = jnp.where(lane == j, column, factor)
        inverse = jnp.where(sub == j, root, inverse)
        columns[j] = jnp.where(sub > j, column, 0.0)
    factor_ref[...] = factor[:, :bs]

    correction = fold(jnp.dot(pieces(coefficients * inverse_root), basis[...], preferred_element_type=F32), bs)
    steps = [columns[j] * inverse for j in range(bs - 1)]
    for s in range(region):
        part = slice(s * tile, (s + 1) * tile)
        solved = (applied[:, part] - correction[:, part]) * inverse
        for j in range(bs - 1):
            solved = solved - steps[j] * solved[j : j + 1]
        new_ref[:, part] = solved

    for m in range(kinds):
        sent = cols[m].at[pl.ds(0, (nrow - 1) * region)]
        pltpu.make_async_copy(sent, sent, ser_send.at[m]).wait()
    for ref, sem in (
        (seg_in, seg_send), (corr_col, cc_send), (inbox, box_send), (corr_row, cr_send), (tail, tail_send)
    ):
        landed(ref, sem)


def leave(new_ref, coef_ref, factor_ref, new_hbm, coef_hbm, factor_hbm, sem):
    copies = [
        pltpu.make_async_copy(src, dst, sem.at[i])
        for i, (src, dst) in enumerate(((new_ref, new_hbm), (coef_ref, coef_hbm), (factor_ref, factor_hbm)))
    ]
    for copy in copies:
        copy.start()
    for copy in copies:
        copy.wait()


def shards(basis, expand, tiles, tile_rows, tile_cols):
    nrow = lax.axis_size("row")
    ncol = lax.axis_size("col")
    krylov, length = basis.shape
    kinds, tpd, tile, _ = tiles.shape
    bs = expand.shape[1]
    region = length // tile
    cap = tpd // ncol
    width = -(-tpd * bs // 128) * 128
    dma = pltpu.SemaphoreType.DMA
    band = 16
    lanes = -(-(-(-krylov // band) * krylov) // 128) * 128
    vmem, hbm = pl.BlockSpec(memory_space=pltpu.VMEM), pl.BlockSpec(memory_space=pltpu.HBM)
    shapes = (
        jax.ShapeDtypeStruct((bs, length), F32),
        jax.ShapeDtypeStruct((bs, krylov), F32),
        jax.ShapeDtypeStruct((bs, bs), F32),
    )
    held = pl.pallas_call(
        functools.partial(kernel, nrow, ncol),
        out_shape=shapes,
        in_specs=[hbm] * 5,
        out_specs=(vmem, vmem, vmem),
        scratch_shapes=[
            pltpu.VMEM(expand.shape, F32),
            pltpu.SMEM((tpd,), jnp.int32),
            pltpu.SMEM((tpd,), jnp.int32),
            pltpu.VMEM((krylov, length), BF16),
            pltpu.VMEM((kinds, tpd, tile, tile), BF16),
            *[pltpu.VMEM((nrow * region, bs, tile), BF16)] * kinds,
            pltpu.VMEM((ncol, cap * bs, tile), BF16),
            pltpu.VMEM((ncol, cap * bs, tile), BF16),
            pltpu.VMEM((ncol, 1, width), jnp.int32),
            pltpu.VMEM((ncol, 1, width), jnp.int32),
            pltpu.VMEM((ncol, band, lanes), F32),
            pltpu.VMEM((nrow, band, lanes), F32),
            pltpu.VMEM((nrow * ncol, bs // 2, 128), F32),
            pltpu.VMEM((region * bs, tpd * bs), BF16),
            pltpu.VMEM((2, cap * bs, tile), F32),
            dma((3,)),
            dma,
            dma((kinds,)),
            dma((kinds,)),
            dma((kinds, nrow // 2)),
            dma((kinds, 2, nrow // 2 - 1)),
        ]
        + [dma] * 10
        + [pltpu.SemaphoreType.REGULAR((max(ncol // 2 - 2, 1),))] * 2,
        compiler_params=pltpu.CompilerParams(
            collective_id=0, has_side_effects=True, vmem_limit_bytes=48 * 1024 * 1024
        ),
    )(*(pltpu.with_memory_space_constraint(x, pltpu.HBM) for x in (expand, tile_rows, tile_cols, basis, tiles)))
    return pl.pallas_call(
        leave,
        out_shape=shapes,
        in_specs=[vmem] * 3,
        out_specs=(hbm, hbm, hbm),
        scratch_shapes=[dma((3,))],
    )(*(pltpu.with_memory_space_constraint(x, pltpu.VMEM) for x in held))


def solution(mesh):
    return jax.shard_map(
        shards,
        mesh=mesh,
        in_specs=(
            P(None, ("row", "col")),
            P(),
            P(None, ("row", "col"), None, None),
            P(("row", "col")),
            P(("row", "col")),
        ),
        out_specs=(P(None, ("row", "col")), P(), P()),
        check_vma=False,
    )
```

```python
import functools
import math

import jax
import jax.numpy as jnp
from jax import lax
from jax.experimental import pallas as pl
from jax.experimental.pallas import tpu as pltpu
from jax.sharding import PartitionSpec as P

F32 = jnp.float32
BF16 = jnp.bfloat16
NT = (((1,), (1,)), ((), ()))


def exact(a, b, dims=(((1,), (0,)), ((), ()))):
    return lax.dot_general(a, b, dims, precision=lax.Precision.HIGHEST, preferred_element_type=F32)


def pieces(x):
    one = x.astype(BF16).astype(F32)
    return jnp.concatenate([one, x - one], axis=0).astype(BF16)


def fold(x, rows):
    return x[:rows] + x[rows:]


def kernel(
    nrow,
    ncol,
    expand_hbm,
    rows_hbm,
    picks_hbm,
    basis_hbm,
    tiles_hbm,
    new_ref,
    coef_ref,
    factor_ref,
    expand_ref,
    rows_ref,
    picks_ref,
    basis,
    tiles,
    cols0,
    cols1,
    cols2,
    outbox,
    inbox,
    seg_out,
    seg_in,
    corr_col,
    corr_row,
    tail,
    place,
    held,
    small_sem,
    basis_sem,
    tile_sem,
    ser_send,
    ser_recv,
    fwd_recv,
    seg_send,
    seg_recv,
    box_send,
    box_recv,
    cc_send,
    cc_recv,
    cr_send,
    cr_recv,
    tail_send,
    tail_recv,
    low_sem,
    high_sem,
):
    r = lax.axis_index("row")
    c = lax.axis_index("col")
    cols = (cols0, cols1, cols2)
    krylov, length = basis.shape
    kinds, tpd, tile, _ = tiles.shape
    cap = tpd // ncol
    region = length // tile
    bs = expand_ref.shape[1]
    entries = length * nrow * ncol
    inverse_root = 1.0 / math.sqrt(entries)
    width = seg_in.shape[2]

    load_basis = pltpu.make_async_copy(basis_hbm, basis, basis_sem)
    load_basis.start()
    small = [
        pltpu.make_async_copy(src, dst, small_sem.at[i])
        for i, (src, dst) in enumerate(((expand_hbm, expand_ref), (rows_hbm, rows_ref), (picks_hbm, picks_ref)))
    ]
    for copy in small:
        copy.start()

    outer = nrow // 2
    side, pair = lax.rem(r, 2), lax.div(r, 2)
    mate = r + 1 - 2 * side
    half = region // 2

    def other(j):
        return 2 * lax.rem(pair + j, outer) + side

    def signal(sem, where):
        pl.semaphore_signal(sem, inc=1, device_id=where, device_id_type=pl.DeviceIdType.MESH)

    barrier = pltpu.get_barrier_semaphore()
    has_low, has_high = c >= 2, c < ncol - 2
    even = c - lax.rem(c, 2)

    def low(i):
        return {"col": lax.rem(even - 2 + i + ncol, ncol)}

    def high(i):
        return {"col": lax.rem(even + 2 + i, ncol)}

    signal(barrier, {"row": mate})
    for j in range(1, outer):
        signal(barrier, {"row": other(j)})
    signal(barrier, {"col": c + 1 - 2 * lax.rem(c, 2)})
    for i in range(2):
        pl.when(has_low)(lambda: signal(barrier, low(i)))
        pl.when(has_high)(lambda: signal(barrier, high(i)))

    def tell(i):
        pl.when(has_low)(lambda: signal(high_sem.at[i], low(lax.rem(c, 2))))
        pl.when(has_high)(lambda: signal(low_sem.at[i], high(lax.rem(c, 2))))

    def hear(i):
        pl.when(has_low)(lambda: pl.semaphore_wait(low_sem.at[i], 1))
        pl.when(has_high)(lambda: pl.semaphore_wait(high_sem.at[i], 1))

    def remote(src, dst, send_sem, recv_sem, where):
        return pltpu.make_async_remote_copy(
            src_ref=src, dst_ref=dst, send_sem=send_sem, recv_sem=recv_sem,
            device_id=where, device_id_type=pl.DeviceIdType.MESH,
        )

    def landed(ref, sem):
        part = ref.at[pl.ds(0, ref.shape[0] - 1)]
        pltpu.make_async_copy(part, part, sem).wait()

    def row_at(j):
        peer = lax.rem(r + j, nrow)
        return peer, {"row": peer}

    def col_at(j):
        peer = lax.rem(c + j, ncol)
        return peer, {"col": peer}

    small[0].wait()
    load_basis.wait()
    for m in range(kinds):
        for k in range(ncol):
            part = pl.ds(k * cap, cap)
            pltpu.make_async_copy(tiles_hbm.at[m, part], tiles.at[m, part], tile_sem.at[m]).start()

    def make(m):
        one = pieces(expand_ref[m])
        for l in range(region):
            part = jnp.dot(one, basis[:, l * tile : (l + 1) * tile], preferred_element_type=F32)
            cols[m][r * region + l] = fold(part, bs).astype(BF16)

    def block(m, owner, h):
        return cols[m].at[pl.ds(owner * region + h * half, half)]

    def series_copy(m, owner, h, peer, slot):
        part = block(m, owner, h)
        return remote(part, part, ser_send.at[m], ser_recv.at[m, h, slot], {"row": peer})

    def pass_on(m, owner, h, peer, slot):
        part = block(m, owner, h)
        return remote(part, part, ser_send.at[m], fwd_recv.at[m, h, slot - 1], {"row": peer})

    def spread(m, h):
        series_copy(m, r, 1 - h, mate, 0).start()
        for j in range(1, outer):
            series_copy(m, r, h, other(j), outer - j).start()

    make(0)

    pl.semaphore_wait(barrier, outer + 1 + 2 * (has_low.astype(jnp.int32) + has_high.astype(jnp.int32)))
    spread(0, 0)
    rounds = ncol // 2 - 2
    if rounds > 0:
        tell(0)

    for m in range(1, kinds):
        make(m)
        spread(m, 0)

    def second_halves():
        for m in range(kinds):
            spread(m, 1)

    late = lax.rem(c, 2) == 1
    pl.when(jnp.logical_not(late))(second_halves)

    small[1].wait()
    small[2].wait()
    slot = lax.broadcasted_iota(jnp.int32, (1, width), 1)
    entry, inner = lax.rem(lax.div(slot, bs), cap), lax.rem(slot, bs)
    for k in range(ncol):
        line = jnp.zeros((1, width), jnp.int32)
        for t in range(cap):
            line = jnp.where(entry == t, rows_ref[k * cap + t] * bs, line)
        seg_out[k] = line + inner
    seg_in[c] = seg_out[c]

    corr = lax.dot_general(basis[...], basis[...], NT, preferred_element_type=F32)
    band = corr_col.shape[1]
    lanes = corr_col.shape[2]
    folds = -(-krylov // band)
    corr = jnp.pad(corr, ((0, folds * band - krylov), (0, 0)))
    corr_col[c] = jnp.concatenate(
        [corr[i * band : (i + 1) * band] for i in range(folds)] + [jnp.zeros((band, lanes - folds * krylov), F32)], axis=1
    )

    def relay(m):
        series_copy(m, mate, 1, mate, 0).wait_recv()
        for j in range(1, outer):
            pass_on(m, mate, 1, other(j), outer - j).start()
        for j in range(1, outer):
            series_copy(m, other(j), 0, other(j), j).wait_recv()
            pass_on(m, other(j), 0, mate, j).start()

    def relayed(m):
        series_copy(m, mate, 0, mate, 0).wait_recv()
        for j in range(1, outer):
            series_copy(m, other(j), 1, other(j), j).wait_recv()
        for j in range(1, outer):
            far = other(j) + 1 - 2 * side
            pass_on(m, far, 0, mate, j).wait_recv()
            pass_on(m, far, 1, mate, j).wait_recv()

    relay(0)
    pl.when(late)(second_halves)
    for i in range(rounds - 1):
        hear(i)
        tell(i + 1)
    relay(1)
    if rounds > 0:
        hear(rounds - 1)
    for j in range(1, ncol):
        peer, where = col_at(j)
        remote(seg_out.at[peer], seg_in.at[c], seg_send, seg_recv, where).start()
    for j in range(1, ncol):
        peer, where = col_at(j)
        remote(corr_col.at[c], corr_col.at[c], cc_send, cc_recv, where).start()
    for m in range(2, kinds):
        relay(m)
    for m in range(kinds - 1):
        relayed(m)

    for m in range(kinds):
        pltpu.make_async_copy(tiles_hbm.at[m], tiles.at[m], tile_sem.at[m]).wait()

    def products(k, t, ms):
        out = []
        for g in (k * cap + t, k * cap + t + 1):
            at = picks_ref[g]
            x = jnp.concatenate([cols[m][at] for m in ms], axis=1)
            w = jnp.concatenate([tiles[m, g] for m in ms], axis=1)
            out.append(lax.dot_general(x, w, NT, preferred_element_type=F32))
        return jnp.concatenate(out, axis=0)

    def box_copy(k):
        return remote(outbox.at[k], inbox.at[c], box_send, box_recv, {"col": k})

    across = ncol // 2
    mine = lax.div(c, across)

    def far_side(i):
        return (1 - mine) * across + lax.rem(c + i, across)

    def near_side(i):
        return mine * across + lax.rem(c + i, across)

    early = held.shape[0]
    for i in range(early):
        for t in range(0, cap, 2):
            held[i, t * bs : (t + 2) * bs] = products(far_side(i), t, range(kinds - 1))

    relayed(kinds - 1)

    for i in range(early):
        k = far_side(i)
        for t in range(0, cap, 2):
            rows = slice(t * bs, (t + 2) * bs)
            outbox[k, rows] = (held[i, rows] + products(k, t, (kinds - 1,))).astype(BF16)
        box_copy(k).start()

    def whole(k, dst):
        for t in range(0, cap, 2):
            dst[k, t * bs : (t + 2) * bs] = products(k, t, range(kinds)).astype(BF16)

    def send_far(i, carry):
        whole(far_side(i), outbox)
        box_copy(far_side(i)).start()
        return carry

    def send_near(i, carry):
        whole(near_side(i), outbox)
        box_copy(near_side(i)).start()
        return carry

    lax.fori_loop(early, across, send_far, 0)
    lax.fori_loop(1, across, send_near, 0)

    whole(c, inbox)

    landed(corr_col, cc_recv)
    corr_row[r] = jnp.sum(corr_col[...], axis=0)
    for j in range(1, nrow):
        peer, where = row_at(j)
        remote(corr_row.at[r], corr_row.at[r], cr_send, cr_recv, where).start()
    landed(seg_in, seg_recv)
    line = seg_in[0]
    for k in range(1, ncol):
        line = jnp.where(lax.div(slot, cap * bs) == k, seg_in[k], line)
    here = lax.broadcasted_iota(jnp.int32, (region * bs, tpd * bs), 0) + c * (region * bs)
    place[...] = (line[:, : tpd * bs] == here).astype(F32).astype(BF16)

    landed(inbox, box_recv)
    app = jnp.dot(place[...], inbox[...].reshape(tpd * bs, tile), preferred_element_type=F32)
    applied = jnp.concatenate([app[s * bs : (s + 1) * bs] for s in range(region)], axis=1)

    split = pieces(applied)
    stack = jnp.concatenate([split, basis[...]], axis=0)
    raw = fold(lax.dot_general(split, stack, NT, preferred_element_type=F32), bs)
    raw = jnp.concatenate([raw, jnp.zeros((bs, 64 - 2 * bs - krylov), F32)], axis=1)
    me = r * ncol + c
    tail[me] = jnp.concatenate([raw[: bs // 2], raw[bs // 2 :]], axis=1)

    for j in sorted(range(ncol), key=lambda j: -min(j, ncol - j)):
        for i in reversed(range(nrow)):
            if i or j:
                where = {"row": lax.rem(r + i, nrow), "col": lax.rem(c + j, ncol)}
                remote(tail.at[me], tail.at[me], tail_send, tail_recv, where).start()

    landed(corr_row, cr_recv)
    corr = jnp.sum(corr_row[...], axis=0) / entries
    corr = jnp.concatenate([corr[:, i * krylov : (i + 1) * krylov] for i in range(folds)], axis=0)[:krylov]
    eye = (
        lax.broadcasted_iota(jnp.int32, (krylov, krylov), 0) == lax.broadcasted_iota(jnp.int32, (krylov, krylov), 1)
    ).astype(F32)
    once = eye - corr
    both = eye + once
    kern = exact(both, eye + exact(once, once)) * (inverse_root / entries * inverse_root)
    before, after = 2 * bs, 64 - 2 * bs - krylov
    down, along = (lax.broadcasted_iota(jnp.int32, (64, bs), d) for d in (0, 1))
    gather = ((down == along) | (down == along + bs)).astype(F32) / entries
    mix = jnp.concatenate(
        [
            jnp.pad(both * inverse_root, ((before, after), (0, 0))),
            gather,
            jnp.zeros((64, 64 + before - krylov - bs), F32),
            jnp.pad(kern, ((before, after), (0, after))),
        ],
        axis=1,
    )
    mix = jnp.concatenate([mix, jnp.zeros((64, 128), F32)], axis=0)
    coarse = mix.astype(BF16).astype(F32)
    mix = jnp.concatenate([coarse, mix - coarse], axis=1).astype(BF16)
    right = lax.broadcasted_iota(jnp.int32, (bs, 128), 1) >= 64
    below = lax.broadcasted_iota(jnp.int32, (bs, 128), 0) >= bs // 2

    landed(tail, tail_recv)

    total = jnp.sum(tail[...], axis=0)
    turned = jnp.concatenate([total[:, 64:], total[:, :64]], axis=1)
    total = jnp.where(right == below, jnp.concatenate([total, total], axis=0), jnp.concatenate([turned, turned], axis=0))
    total = pieces(total)
    made = fold(jnp.dot(total, mix, preferred_element_type=F32), bs)
    made = made[:, :128] + made[:, 128:]
    taken = pieces(jnp.where(right, made, 0.0))
    taken = fold(lax.dot_general(taken, total, NT, preferred_element_type=F32), bs)
    gram = made[:, krylov : krylov + bs] - (taken[:, :bs] + taken[:, bs:])
    coefficients = made[:, :krylov]
    coef_ref[...] = coefficients

    sub = lax.broadcasted_iota(jnp.int32, (bs, tile), 0)
    lane = lax.broadcasted_iota(jnp.int32, (bs, tile), 1)
    columns = [jnp.broadcast_to(gram[:, j : j + 1], (bs, tile)) for j in range(bs)]
    factor = jnp.zeros((bs, tile), F32)
    inverse = jnp.zeros((bs, tile), F32)
    for j in range(bs):
        root = jnp.broadcast_to(lax.rsqrt(columns[j][j : j + 1]), (bs, tile))
        column = jnp.where(sub >= j, columns[j] * root, 0.0)
        for k in range(j + 1, bs):
            columns[k] = columns[k] - column * column[k : k + 1]
        factor = jnp.where(lane == j, column, factor)
        inverse = jnp.where(sub == j, root, inverse)
        columns[j] = jnp.where(sub > j, column, 0.0)
    factor_ref[...] = factor[:, :bs]

    correction = fold(jnp.dot(pieces(coefficients * inverse_root), basis[...], preferred_element_type=F32), bs)
    steps = [columns[j] * inverse for j in range(bs - 1)]
    for s in range(region):
        part = slice(s * tile, (s + 1) * tile)
        solved = (applied[:, part] - correction[:, part]) * inverse
        for j in range(bs - 1):
            solved = solved - steps[j] * solved[j : j + 1]
        new_ref[:, part] = solved

    for m in range(kinds):
        sent = cols[m].at[pl.ds(0, (nrow - 1) * region)]
        pltpu.make_async_copy(sent, sent, ser_send.at[m]).wait()
    for ref, sem in (
        (seg_in, seg_send), (corr_col, cc_send), (inbox, box_send), (corr_row, cr_send), (tail, tail_send)
    ):
        landed(ref, sem)


def leave(new_ref, coef_ref, factor_ref, new_hbm, coef_hbm, factor_hbm, sem):
    copies = [
        pltpu.make_async_copy(src, dst, sem.at[i])
        for i, (src, dst) in enumerate(((new_ref, new_hbm), (coef_ref, coef_hbm), (factor_ref, factor_hbm)))
    ]
    for copy in copies:
        copy.start()
    for copy in copies:
        copy.wait()


def shards(basis, expand, tiles, tile_rows, tile_cols):
    nrow = lax.axis_size("row")
    ncol = lax.axis_size("col")
    krylov, length = basis.shape
    kinds, tpd, tile, _ = tiles.shape
    bs = expand.shape[1]
    region = length // tile
    cap = tpd // ncol
    width = -(-tpd * bs // 128) * 128
    dma = pltpu.SemaphoreType.DMA
    band = 16
    lanes = -(-(-(-krylov // band) * krylov) // 128) * 128
    vmem, hbm = pl.BlockSpec(memory_space=pltpu.VMEM), pl.BlockSpec(memory_space=pltpu.HBM)
    shapes = (
        jax.ShapeDtypeStruct((bs, length), F32),
        jax.ShapeDtypeStruct((bs, krylov), F32),
        jax.ShapeDtypeStruct((bs, bs), F32),
    )
    held = pl.pallas_call(
        functools.partial(kernel, nrow, ncol),
        out_shape=shapes,
        in_specs=[hbm] * 5,
        out_specs=(vmem, vmem, vmem),
        scratch_shapes=[
            pltpu.VMEM(expand.shape, F32),
            pltpu.SMEM((tpd,), jnp.int32),
            pltpu.SMEM((tpd,), jnp.int32),
            pltpu.VMEM((krylov, length), BF16),
            pltpu.VMEM((kinds, tpd, tile, tile), BF16),
            *[pltpu.VMEM((nrow * region, bs, tile), BF16)] * kinds,
            pltpu.VMEM((ncol, cap * bs, tile), BF16),
            pltpu.VMEM((ncol, cap * bs, tile), BF16),
            pltpu.VMEM((ncol, 1, width), jnp.int32),
            pltpu.VMEM((ncol, 1, width), jnp.int32),
            pltpu.VMEM((ncol, band, lanes), F32),
            pltpu.VMEM((nrow, band, lanes), F32),
            pltpu.VMEM((nrow * ncol, bs // 2, 128), F32),
            pltpu.VMEM((region * bs, tpd * bs), BF16),
            pltpu.VMEM((2, cap * bs, tile), F32),
            dma((3,)),
            dma,
            dma((kinds,)),
            dma((kinds,)),
            dma((kinds, 2, nrow // 2)),
            dma((kinds, 2, nrow // 2 - 1)),
        ]
        + [dma] * 10
        + [pltpu.SemaphoreType.REGULAR((max(ncol // 2 - 2, 1),))] * 2,
        compiler_params=pltpu.CompilerParams(
            collective_id=0, has_side_effects=True, vmem_limit_bytes=48 * 1024 * 1024
        ),
    )(*(pltpu.with_memory_space_constraint(x, pltpu.HBM) for x in (expand, tile_rows, tile_cols, basis, tiles)))
    return pl.pallas_call(
        leave,
        out_shape=shapes,
        in_specs=[vmem] * 3,
        out_specs=(hbm, hbm, hbm),
        scratch_shapes=[dma((3,))],
    )(*(pltpu.with_memory_space_constraint(x, pltpu.VMEM) for x in held))


def solution(mesh):
    return jax.shard_map(
        shards,
        mesh=mesh,
        in_specs=(
            P(None, ("row", "col")),
            P(),
            P(None, ("row", "col"), None, None),
            P(("row", "col")),
            P(("row", "col")),
        ),
        out_specs=(P(None, ("row", "col")), P(), P()),
        check_vma=False,
    )
```

```python
import functools
import math

import jax
import jax.numpy as jnp
from jax import lax
from jax.experimental import pallas as pl
from jax.experimental.pallas import tpu as pltpu
from jax.sharding import PartitionSpec as P

F32 = jnp.float32
BF16 = jnp.bfloat16
NT = (((1,), (1,)), ((), ()))


def exact(a, b, dims=(((1,), (0,)), ((), ()))):
    return lax.dot_general(a, b, dims, precision=lax.Precision.HIGHEST, preferred_element_type=F32)


def pieces(x):
    one = x.astype(BF16).astype(F32)
    return jnp.concatenate([one, x - one], axis=0).astype(BF16)


def fold(x, rows):
    return x[:rows] + x[rows:]


def kernel(
    nrow,
    ncol,
    expand_hbm,
    rows_hbm,
    picks_hbm,
    basis_hbm,
    tiles_hbm,
    new_ref,
    coef_ref,
    factor_ref,
    expand_ref,
    rows_ref,
    picks_ref,
    basis,
    tiles,
    cols0,
    cols1,
    cols2,
    outbox,
    inbox,
    seg_out,
    seg_in,
    corr_col,
    corr_row,
    tail,
    place,
    held,
    small_sem,
    basis_sem,
    tile_sem,
    ser_send,
    ser_recv,
    rest_recv,
    seg_send,
    seg_recv,
    box_send,
    box_recv,
    cc_send,
    cc_recv,
    cr_send,
    cr_recv,
    tail_send,
    tail_recv,
    low_sem,
    high_sem,
):
    r = lax.axis_index("row")
    c = lax.axis_index("col")
    cols = (cols0, cols1, cols2)
    krylov, length = basis.shape
    kinds, tpd, tile, _ = tiles.shape
    cap = tpd // ncol
    region = length // tile
    bs = expand_ref.shape[1]
    entries = length * nrow * ncol
    inverse_root = 1.0 / math.sqrt(entries)
    width = seg_in.shape[2]

    parts = 4
    for i in range(parts):
        part = pl.ds(i * (length // parts), length // parts)
        pltpu.make_async_copy(basis_hbm.at[:, part], basis.at[:, part], basis_sem).start()
    small = [
        pltpu.make_async_copy(src, dst, small_sem.at[i])
        for i, (src, dst) in enumerate(((expand_hbm, expand_ref), (rows_hbm, rows_ref), (picks_hbm, picks_ref)))
    ]
    for copy in small:
        copy.start()

    outer = nrow // 2
    side, pair = lax.rem(r, 2), lax.div(r, 2)
    mate = r + 1 - 2 * side
    half = region // 2

    def other(j):
        return 2 * lax.rem(pair + j, outer) + side

    def signal(sem, where):
        pl.semaphore_signal(sem, inc=1, device_id=where, device_id_type=pl.DeviceIdType.MESH)

    barrier = pltpu.get_barrier_semaphore()
    has_low, has_high = c >= 2, c < ncol - 2
    even = c - lax.rem(c, 2)

    def low(i):
        return {"col": lax.rem(even - 2 + i + ncol, ncol)}

    def high(i):
        return {"col": lax.rem(even + 2 + i, ncol)}

    signal(barrier, {"row": mate})
    for j in range(1, outer):
        signal(barrier, {"row": other(j)})
    signal(barrier, {"col": c + 1 - 2 * lax.rem(c, 2)})
    for i in range(2):
        pl.when(has_low)(lambda: signal(barrier, low(i)))
        pl.when(has_high)(lambda: signal(barrier, high(i)))

    def tell(i):
        pl.when(has_low)(lambda: signal(high_sem.at[i], low(lax.rem(c, 2))))
        pl.when(has_high)(lambda: signal(low_sem.at[i], high(lax.rem(c, 2))))

    def hear(i):
        pl.when(has_low)(lambda: pl.semaphore_wait(low_sem.at[i], 1))
        pl.when(has_high)(lambda: pl.semaphore_wait(high_sem.at[i], 1))

    def remote(src, dst, send_sem, recv_sem, where):
        return pltpu.make_async_remote_copy(
            src_ref=src, dst_ref=dst, send_sem=send_sem, recv_sem=recv_sem,
            device_id=where, device_id_type=pl.DeviceIdType.MESH,
        )

    def landed(ref, sem):
        part = ref.at[pl.ds(0, ref.shape[0] - 1)]
        pltpu.make_async_copy(part, part, sem).wait()

    def row_at(j):
        peer = lax.rem(r + j, nrow)
        return peer, {"row": peer}

    def col_at(j):
        peer = lax.rem(c + j, ncol)
        return peer, {"col": peer}

    small[0].wait()
    pltpu.make_async_copy(basis_hbm, basis, basis_sem).wait()
    for m in range(kinds):
        for k in range(ncol):
            part = pl.ds(k * cap, cap)
            pltpu.make_async_copy(tiles_hbm.at[m, part], tiles.at[m, part], tile_sem).start()

    def make(m):
        one = pieces(expand_ref[m])
        for l in range(region):
            part = jnp.dot(one, basis[:, l * tile : (l + 1) * tile], preferred_element_type=F32)
            cols[m][r * region + l] = fold(part, bs).astype(BF16)

    def block(m, owner, h):
        return cols[m].at[pl.ds(owner * region + h * half, half)]

    def first_half(m, owner, h, peer, slot):
        part = block(m, owner, h)
        return remote(part, part, ser_send.at[m], ser_recv.at[m, slot], {"row": peer})

    def send_rest(m, owner, h, peer):
        part = block(m, owner, h)
        remote(part, part, ser_send.at[m], rest_recv.at[m], {"row": peer}).start()

    def spread(m):
        first_half(m, r, 1, mate, 0).start()
        for j in range(1, outer):
            first_half(m, r, 0, other(j), outer - j).start()

    make(0)

    pl.semaphore_wait(barrier, outer + 1 + 2 * (has_low.astype(jnp.int32) + has_high.astype(jnp.int32)))
    spread(0)
    rounds = ncol // 2 - 2
    if rounds > 0:
        tell(0)

    for m in range(1, kinds):
        make(m)
        spread(m)

    for m in range(kinds):
        send_rest(m, r, 0, mate)
        for j in range(1, outer):
            send_rest(m, r, 1, other(j))

    small[1].wait()
    small[2].wait()
    slot = lax.broadcasted_iota(jnp.int32, (1, width), 1)
    entry, inner = lax.rem(lax.div(slot, bs), cap), lax.rem(slot, bs)
    for k in range(ncol):
        line = jnp.zeros((1, width), jnp.int32)
        for t in range(cap):
            line = jnp.where(entry == t, rows_ref[k * cap + t] * bs, line)
        seg_out[k] = line + inner
    seg_in[c] = seg_out[c]

    corr = lax.dot_general(basis[...], basis[...], NT, preferred_element_type=F32)
    band = corr_col.shape[1]
    lanes = corr_col.shape[2]
    folds = -(-krylov // band)
    corr = jnp.pad(corr, ((0, folds * band - krylov), (0, 0)))
    corr_col[c] = jnp.concatenate(
        [corr[i * band : (i + 1) * band] for i in range(folds)] + [jnp.zeros((band, lanes - folds * krylov), F32)], axis=1
    )

    def relay(m):
        first_half(m, mate, 1, mate, 0).wait_recv()
        for j in range(1, outer):
            send_rest(m, mate, 1, other(j))
        for j in range(1, outer):
            first_half(m, other(j), 0, other(j), j).wait_recv()
            send_rest(m, other(j), 0, mate)

    def relayed(m):
        rest = cols[m].at[pl.ds(0, (3 * outer - 2) * half)]
        pltpu.make_async_copy(rest, rest, rest_recv.at[m]).wait()

    relay(0)
    for i in range(rounds - 1):
        hear(i)
        tell(i + 1)
    relay(1)
    if rounds > 0:
        hear(rounds - 1)
    for j in range(1, ncol):
        peer, where = col_at(j)
        remote(seg_out.at[peer], seg_in.at[c], seg_send, seg_recv, where).start()
    for j in range(1, ncol):
        peer, where = col_at(j)
        remote(corr_col.at[c], corr_col.at[c], cc_send, cc_recv, where).start()
    for m in range(2, kinds):
        relay(m)
    for m in range(kinds - 1):
        relayed(m)

    pltpu.make_async_copy(tiles_hbm, tiles, tile_sem).wait()

    def products(k, t, ms):
        out = []
        for g in (k * cap + t, k * cap + t + 1):
            at = picks_ref[g]
            x = jnp.concatenate([cols[m][at] for m in ms], axis=1)
            w = jnp.concatenate([tiles[m, g] for m in ms], axis=1)
            out.append(lax.dot_general(x, w, NT, preferred_element_type=F32))
        return jnp.concatenate(out, axis=0)

    def box_copy(k):
        return remote(outbox.at[k], inbox.at[c], box_send, box_recv, {"col": k})

    across = ncol // 2
    mine = lax.div(c, across)

    upper = mine == 1

    def far_side(i):
        return jnp.where(upper, i, ncol - 2 - 2 * lax.div(i, 2) + lax.rem(i, 2))

    def near_side(i):
        step = jnp.where(lax.rem(c, 2) == 1, i, lax.rem(i, across - 1) + 1)
        return mine * across + lax.rem(c + step, across)

    early = held.shape[0]
    for i in range(early):
        for t in range(0, cap, 2):
            held[i, t * bs : (t + 2) * bs] = products(far_side(jnp.int32(i)), t, range(kinds - 1))

    relayed(kinds - 1)

    for i in range(early):
        k = far_side(jnp.int32(i))
        for t in range(0, cap, 2):
            rows = slice(t * bs, (t + 2) * bs)
            outbox[k, rows] = (held[i, rows] + products(k, t, (kinds - 1,))).astype(BF16)
        box_copy(k).start()

    def whole(k, dst):
        for t in range(0, cap, 2):
            dst[k, t * bs : (t + 2) * bs] = products(k, t, range(kinds)).astype(BF16)

    def send_far(i, carry):
        whole(far_side(i), outbox)
        box_copy(far_side(i)).start()
        return carry

    def send_near(i, carry):
        whole(near_side(i), outbox)
        box_copy(near_side(i)).start()
        return carry

    lax.fori_loop(early, across, send_far, 0)
    lax.fori_loop(1, across, send_near, 0)

    whole(c, inbox)

    landed(corr_col, cc_recv)
    corr_row[r] = jnp.sum(corr_col[...], axis=0)
    for j in range(1, nrow):
        peer, where = row_at(j)
        remote(corr_row.at[r], corr_row.at[r], cr_send, cr_recv, where).start()
    landed(seg_in, seg_recv)
    line = seg_in[0]
    for k in range(1, ncol):
        line = jnp.where(lax.div(slot, cap * bs) == k, seg_in[k], line)
    here = lax.broadcasted_iota(jnp.int32, (region * bs, tpd * bs), 0) + c * (region * bs)
    place[...] = (line[:, : tpd * bs] == here).astype(F32).astype(BF16)

    landed(inbox, box_recv)
    app = jnp.dot(place[...], inbox[...].reshape(tpd * bs, tile), preferred_element_type=F32)
    applied = jnp.concatenate([app[s * bs : (s + 1) * bs] for s in range(region)], axis=1)

    split = pieces(applied)
    stack = jnp.concatenate([split, basis[...]], axis=0)
    raw = fold(lax.dot_general(split, stack, NT, preferred_element_type=F32), bs)
    raw = jnp.concatenate([raw, jnp.zeros((bs, 64 - 2 * bs - krylov), F32)], axis=1)
    me = r * ncol + c
    tail[me] = jnp.concatenate([raw[: bs // 2], raw[bs // 2 :]], axis=1)

    columns = [far_side(jnp.int32(i)) for i in range(across)] + [near_side(jnp.int32(i)) for i in range(1, across)]
    for k in columns + [c]:
        for i in reversed(range(1 if k is c else 0, nrow)):
            where = {"row": lax.rem(r + i, nrow), "col": k}
            remote(tail.at[me], tail.at[me], tail_send, tail_recv, where).start()

    landed(corr_row, cr_recv)
    corr = jnp.sum(corr_row[...], axis=0) / entries
    corr = jnp.concatenate([corr[:, i * krylov : (i + 1) * krylov] for i in range(folds)], axis=0)[:krylov]
    eye = (
        lax.broadcasted_iota(jnp.int32, (krylov, krylov), 0) == lax.broadcasted_iota(jnp.int32, (krylov, krylov), 1)
    ).astype(F32)
    once = eye - corr
    both = eye + once
    kern = exact(both, eye + exact(once, once)) * (inverse_root / entries * inverse_root)
    before, after = 2 * bs, 64 - 2 * bs - krylov
    down, along = (lax.broadcasted_iota(jnp.int32, (64, bs), d) for d in (0, 1))
    gather = ((down == along) | (down == along + bs)).astype(F32) / entries
    narrow = jnp.concatenate(
        [jnp.pad(both * inverse_root, ((before, after), (0, 0))), gather, jnp.zeros((64, 128 - krylov - bs), F32)], axis=1
    )
    kern = jnp.pad(kern, ((before, after), (before, after)))
    mix = jnp.concatenate([kern, kern, narrow], axis=1)
    mix = jnp.concatenate([mix, jnp.zeros((64, 256), F32)], axis=0)
    coarse = mix.astype(BF16).astype(F32)
    mix = jnp.concatenate([coarse, mix - coarse], axis=1).astype(BF16)
    right = lax.broadcasted_iota(jnp.int32, (bs, 128), 1) >= 64
    below = lax.broadcasted_iota(jnp.int32, (bs, 128), 0) >= bs // 2

    landed(tail, tail_recv)

    total = jnp.sum(tail[...], axis=0)
    turned = jnp.concatenate([total[:, 64:], total[:, :64]], axis=1)
    total = jnp.where(right == below, jnp.concatenate([total, total], axis=0), jnp.concatenate([turned, turned], axis=0))
    lead = total.astype(BF16).astype(F32)
    made = fold(jnp.dot(pieces(total), mix, preferred_element_type=F32), bs)
    taken, made = made[:, :128] + made[:, 256:384], made[:, 128:256] + made[:, 384:]
    total = jnp.where(right, total - lead, lead).astype(BF16)
    gram = made[:, krylov : krylov + bs] - fold(lax.dot_general(pieces(taken), total, NT, preferred_element_type=F32), bs)
    coefficients = made[:, :krylov]
    coef_ref[...] = coefficients

    sub = lax.broadcasted_iota(jnp.int32, (bs, tile), 0)
    lane = lax.broadcasted_iota(jnp.int32, (bs, tile), 1)
    columns = [jnp.broadcast_to(gram[:, j : j + 1], (bs, tile)) for j in range(bs)]
    factor = jnp.zeros((bs, tile), F32)
    inverse = jnp.zeros((bs, tile), F32)
    for j in range(bs):
        root = jnp.broadcast_to(lax.rsqrt(columns[j][j : j + 1]), (bs, tile))
        column = jnp.where(sub >= j, columns[j] * root, 0.0)
        for k in range(j + 1, bs):
            columns[k] = columns[k] - column * column[k : k + 1]
        factor = jnp.where(lane == j, column, factor)
        inverse = jnp.where(sub == j, root, inverse)
        columns[j] = jnp.where(sub > j, column, 0.0)
    factor_ref[...] = factor[:, :bs]

    correction = fold(jnp.dot(pieces(coefficients * inverse_root), basis[...], preferred_element_type=F32), bs)
    steps = [columns[j] * inverse for j in range(bs - 1)]
    for s in range(region):
        part = slice(s * tile, (s + 1) * tile)
        solved = (applied[:, part] - correction[:, part]) * inverse
        for j in range(bs - 1):
            solved = solved - steps[j] * solved[j : j + 1]
        new_ref[:, part] = solved

    for m in range(kinds):
        sent = cols[m].at[pl.ds(0, (nrow - 1) * region)]
        pltpu.make_async_copy(sent, sent, ser_send.at[m]).wait()
    for ref, sem in (
        (seg_in, seg_send), (corr_col, cc_send), (inbox, box_send), (corr_row, cr_send), (tail, tail_send)
    ):
        landed(ref, sem)


def leave(new_ref, coef_ref, factor_ref, new_hbm, coef_hbm, factor_hbm, sem):
    copies = [
        pltpu.make_async_copy(src, dst, sem.at[i])
        for i, (src, dst) in enumerate(((new_ref, new_hbm), (coef_ref, coef_hbm), (factor_ref, factor_hbm)))
    ]
    for copy in copies:
        copy.start()
    for copy in copies:
        copy.wait()


def shards(basis, expand, tiles, tile_rows, tile_cols):
    nrow = lax.axis_size("row")
    ncol = lax.axis_size("col")
    krylov, length = basis.shape
    kinds, tpd, tile, _ = tiles.shape
    bs = expand.shape[1]
    region = length // tile
    cap = tpd // ncol
    width = -(-tpd * bs // 128) * 128
    dma = pltpu.SemaphoreType.DMA
    band = 16
    lanes = -(-(-(-krylov // band) * krylov) // 128) * 128
    vmem, hbm = pl.BlockSpec(memory_space=pltpu.VMEM), pl.BlockSpec(memory_space=pltpu.HBM)
    shapes = (
        jax.ShapeDtypeStruct((bs, length), F32),
        jax.ShapeDtypeStruct((bs, krylov), F32),
        jax.ShapeDtypeStruct((bs, bs), F32),
    )
    held = pl.pallas_call(
        functools.partial(kernel, nrow, ncol),
        out_shape=shapes,
        in_specs=[hbm] * 5,
        out_specs=(vmem, vmem, vmem),
        scratch_shapes=[
            pltpu.VMEM(expand.shape, F32),
            pltpu.SMEM((tpd,), jnp.int32),
            pltpu.SMEM((tpd,), jnp.int32),
            pltpu.VMEM((krylov, length), BF16),
            pltpu.VMEM((kinds, tpd, tile, tile), BF16),
            *[pltpu.VMEM((nrow * region, bs, tile), BF16)] * kinds,
            pltpu.VMEM((ncol, cap * bs, tile), BF16),
            pltpu.VMEM((ncol, cap * bs, tile), BF16),
            pltpu.VMEM((ncol, 1, width), jnp.int32),
            pltpu.VMEM((ncol, 1, width), jnp.int32),
            pltpu.VMEM((ncol, band, lanes), F32),
            pltpu.VMEM((nrow, band, lanes), F32),
            pltpu.VMEM((nrow * ncol, bs // 2, 128), F32),
            pltpu.VMEM((region * bs, tpd * bs), BF16),
            pltpu.VMEM((1, cap * bs, tile), F32),
            dma((3,)),
            dma,
            dma,
            dma((kinds,)),
            dma((kinds, nrow // 2)),
            dma((kinds,)),
        ]
        + [dma] * 10
        + [pltpu.SemaphoreType.REGULAR((max(ncol // 2 - 2, 1),))] * 2,
        compiler_params=pltpu.CompilerParams(
            collective_id=0, has_side_effects=True, vmem_limit_bytes=48 * 1024 * 1024
        ),
    )(*(pltpu.with_memory_space_constraint(x, pltpu.HBM) for x in (expand, tile_rows, tile_cols, basis, tiles)))
    return pl.pallas_call(
        leave,
        out_shape=shapes,
        in_specs=[vmem] * 3,
        out_specs=(hbm, hbm, hbm),
        scratch_shapes=[dma((3,))],
    )(*(pltpu.with_memory_space_constraint(x, pltpu.VMEM) for x in held))


def solution(mesh):
    return jax.shard_map(
        shards,
        mesh=mesh,
        in_specs=(
            P(None, ("row", "col")),
            P(),
            P(None, ("row", "col"), None, None),
            P(("row", "col")),
            P(("row", "col")),
        ),
        out_specs=(P(None, ("row", "col")), P(), P()),
        check_vma=False,
    )
```

```python
import functools
import math

import jax
import jax.numpy as jnp
from jax import lax
from jax.experimental import pallas as pl
from jax.experimental.pallas import tpu as pltpu
from jax.sharding import PartitionSpec as P

F32 = jnp.float32
BF16 = jnp.bfloat16
NT = (((1,), (1,)), ((), ()))


def exact(a, b, dims=(((1,), (0,)), ((), ()))):
    return lax.dot_general(a, b, dims, precision=lax.Precision.HIGHEST, preferred_element_type=F32)


def pieces(x):
    one = x.astype(BF16).astype(F32)
    return jnp.concatenate([one, x - one], axis=0).astype(BF16)


def fold(x, rows):
    return x[:rows] + x[rows:]


def kernel(
    nrow,
    ncol,
    expand_hbm,
    rows_hbm,
    picks_hbm,
    basis_hbm,
    tiles_hbm,
    new_ref,
    coef_ref,
    factor_ref,
    expand_ref,
    rows_ref,
    picks_ref,
    basis,
    tiles,
    cols0,
    cols1,
    cols2,
    outbox,
    inbox,
    seg_out,
    seg_in,
    corr_col,
    corr_row,
    tail,
    place,
    held,
    small_sem,
    basis_sem,
    tile_sem,
    ser_send,
    ser_recv,
    rest_recv,
    seg_send,
    seg_recv,
    box_send,
    box_recv,
    cc_send,
    cc_recv,
    cr_send,
    cr_recv,
    tail_send,
    tail_recv,
    low_sem,
    high_sem,
):
    r = lax.axis_index("row")
    c = lax.axis_index("col")
    cols = (cols0, cols1, cols2)
    krylov, length = basis.shape
    kinds, tpd, tile, _ = tiles.shape
    cap = tpd // ncol
    region = length // tile
    bs = expand_ref.shape[1]
    entries = length * nrow * ncol
    inverse_root = 1.0 / math.sqrt(entries)
    width = seg_in.shape[2]

    parts = 4
    for i in range(parts):
        part = pl.ds(i * (length // parts), length // parts)
        pltpu.make_async_copy(basis_hbm.at[:, part], basis.at[:, part], basis_sem).start()
    small = [
        pltpu.make_async_copy(src, dst, small_sem.at[i])
        for i, (src, dst) in enumerate(((expand_hbm, expand_ref), (rows_hbm, rows_ref), (picks_hbm, picks_ref)))
    ]
    for copy in small:
        copy.start()

    outer = nrow // 2
    side, pair = lax.rem(r, 2), lax.div(r, 2)
    mate = r + 1 - 2 * side
    half = region // 2

    def other(j):
        return 2 * lax.rem(pair + j, outer) + side

    def signal(sem, where):
        pl.semaphore_signal(sem, inc=1, device_id=where, device_id_type=pl.DeviceIdType.MESH)

    barrier = pltpu.get_barrier_semaphore()
    has_low, has_high = c >= 2, c < ncol - 2
    even = c - lax.rem(c, 2)

    def low(i):
        return {"col": lax.rem(even - 2 + i + ncol, ncol)}

    def high(i):
        return {"col": lax.rem(even + 2 + i, ncol)}

    signal(barrier, {"row": mate})
    for j in range(1, outer):
        signal(barrier, {"row": other(j)})
    signal(barrier, {"col": c + 1 - 2 * lax.rem(c, 2)})
    for i in range(2):
        pl.when(has_low)(lambda: signal(barrier, low(i)))
        pl.when(has_high)(lambda: signal(barrier, high(i)))

    def tell(i):
        pl.when(has_low)(lambda: signal(high_sem.at[i], low(lax.rem(c, 2))))
        pl.when(has_high)(lambda: signal(low_sem.at[i], high(lax.rem(c, 2))))

    def hear(i):
        pl.when(has_low)(lambda: pl.semaphore_wait(low_sem.at[i], 1))
        pl.when(has_high)(lambda: pl.semaphore_wait(high_sem.at[i], 1))

    def remote(src, dst, send_sem, recv_sem, where):
        return pltpu.make_async_remote_copy(
            src_ref=src, dst_ref=dst, send_sem=send_sem, recv_sem=recv_sem,
            device_id=where, device_id_type=pl.DeviceIdType.MESH,
        )

    def landed(ref, sem):
        part = ref.at[pl.ds(0, ref.shape[0] - 1)]
        pltpu.make_async_copy(part, part, sem).wait()

    def row_at(j):
        peer = lax.rem(r + j, nrow)
        return peer, {"row": peer}

    def col_at(j):
        peer = lax.rem(c + j, ncol)
        return peer, {"col": peer}

    small[0].wait()
    pltpu.make_async_copy(basis_hbm, basis, basis_sem).wait()
    for m in range(kinds):
        for k in range(ncol):
            part = pl.ds(k * cap, cap)
            pltpu.make_async_copy(tiles_hbm.at[m, part], tiles.at[m, part], tile_sem).start()

    def make(m):
        one = pieces(expand_ref[m])
        for l in range(region):
            part = jnp.dot(one, basis[:, l * tile : (l + 1) * tile], preferred_element_type=F32)
            cols[m][r * region + l] = fold(part, bs).astype(BF16)

    def block(m, owner, h):
        return cols[m].at[pl.ds(owner * region + h * half, half)]

    def first_half(m, owner, h, peer, slot):
        part = block(m, owner, h)
        return remote(part, part, ser_send.at[m], ser_recv.at[m, slot], {"row": peer})

    def send_rest(m, owner, h, peer):
        part = block(m, owner, h)
        remote(part, part, ser_send.at[m], rest_recv.at[m], {"row": peer}).start()

    def spread(m):
        first_half(m, r, 1, mate, 0).start()
        for j in range(1, outer):
            first_half(m, r, 0, other(j), outer - j).start()

    make(0)

    pl.semaphore_wait(barrier, outer + 1 + 2 * (has_low.astype(jnp.int32) + has_high.astype(jnp.int32)))
    spread(0)
    rounds = ncol // 2 - 2
    if rounds > 0:
        tell(0)

    for m in range(1, kinds):
        make(m)
        spread(m)

    for m in range(kinds):
        send_rest(m, r, 0, mate)
        for j in range(1, outer):
            send_rest(m, r, 1, other(j))

    small[1].wait()
    small[2].wait()
    slot = lax.broadcasted_iota(jnp.int32, (1, width), 1)
    entry, inner = lax.rem(lax.div(slot, bs), cap), lax.rem(slot, bs)
    for k in range(ncol):
        line = jnp.zeros((1, width), jnp.int32)
        for t in range(cap):
            line = jnp.where(entry == t, rows_ref[k * cap + t] * bs, line)
        seg_out[k] = line + inner
    seg_in[c] = seg_out[c]

    corr = lax.dot_general(basis[...], basis[...], NT, preferred_element_type=F32)
    band = corr_col.shape[1]
    lanes = corr_col.shape[2]
    folds = -(-krylov // band)
    corr = jnp.pad(corr, ((0, folds * band - krylov), (0, 0)))
    corr_col[c] = jnp.concatenate(
        [corr[i * band : (i + 1) * band] for i in range(folds)] + [jnp.zeros((band, lanes - folds * krylov), F32)], axis=1
    )

    def relay(m):
        first_half(m, mate, 1, mate, 0).wait_recv()
        for j in range(1, outer):
            send_rest(m, mate, 1, other(j))
        for j in range(1, outer):
            first_half(m, other(j), 0, other(j), j).wait_recv()
            send_rest(m, other(j), 0, mate)

    def relayed(m):
        rest = cols[m].at[pl.ds(0, (3 * outer - 2) * half)]
        pltpu.make_async_copy(rest, rest, rest_recv.at[m]).wait()

    relay(0)
    for i in range(rounds - 1):
        hear(i)
        tell(i + 1)
    relay(1)
    if rounds > 0:
        hear(rounds - 1)
    for j in range(1, ncol):
        peer, where = col_at(j)
        remote(seg_out.at[peer], seg_in.at[c], seg_send, seg_recv, where).start()
    for j in range(1, ncol):
        peer, where = col_at(j)
        remote(corr_col.at[c], corr_col.at[c], cc_send, cc_recv, where).start()
    for m in range(2, kinds):
        relay(m)
    for m in range(kinds - 1):
        relayed(m)

    pltpu.make_async_copy(tiles_hbm, tiles, tile_sem).wait()

    def products(k, t, ms):
        out = []
        for g in (k * cap + t, k * cap + t + 1):
            at = picks_ref[g]
            x = jnp.concatenate([cols[m][at] for m in ms], axis=1)
            w = jnp.concatenate([tiles[m, g] for m in ms], axis=1)
            out.append(lax.dot_general(x, w, NT, preferred_element_type=F32))
        return jnp.concatenate(out, axis=0)

    def box_copy(k):
        return remote(outbox.at[k], inbox.at[c], box_send, box_recv, {"col": k})

    across = ncol // 2
    mine = lax.div(c, across)

    upper = mine == 1

    def far_side(i):
        return jnp.where(upper, i, ncol - 2 - 2 * lax.div(i, 2) + lax.rem(i, 2))

    def near_side(i):
        step = jnp.where(lax.rem(c, 2) == 1, i, lax.rem(i, across - 1) + 1)
        return mine * across + lax.rem(c + step, across)

    far = [far_side(jnp.int32(i)) for i in range(across)]
    near = [near_side(jnp.int32(i)) for i in range(1, across)]
    early = held.shape[0]
    for i in range(early):
        for t in range(0, cap, 2):
            held[i, t * bs : (t + 2) * bs] = products(far[i], t, range(kinds - 1))

    relayed(kinds - 1)

    def whole(k, dst):
        for t in range(0, cap, 2):
            dst[k, t * bs : (t + 2) * bs] = products(k, t, range(kinds)).astype(BF16)

    for i in range(early):
        for t in range(0, cap, 2):
            rows = slice(t * bs, (t + 2) * bs)
            outbox[far[i], rows] = (held[i, rows] + products(far[i], t, (kinds - 1,))).astype(BF16)
        box_copy(far[i]).start()

    def pick(s):
        others = across - 2
        k = jnp.where(s < others, near_side(s + 1), near_side(jnp.int32(across - 1)))
        at = s - others + early
        return jnp.where((s >= others) & (at < across), far_side(at), k)

    def send(s, carry):
        k = pick(s)
        whole(k, outbox)
        box_copy(k).start()
        return carry

    lax.fori_loop(0, 2 * across - 1 - early, send, 0)
    whole(c, inbox)

    landed(corr_col, cc_recv)
    corr_row[r] = jnp.sum(corr_col[...], axis=0)
    for j in range(1, nrow):
        peer, where = row_at(j)
        remote(corr_row.at[r], corr_row.at[r], cr_send, cr_recv, where).start()
    landed(seg_in, seg_recv)
    line = seg_in[0]
    for k in range(1, ncol):
        line = jnp.where(lax.div(slot, cap * bs) == k, seg_in[k], line)
    here = lax.broadcasted_iota(jnp.int32, (region * bs, tpd * bs), 0) + c * (region * bs)
    place[...] = (line[:, : tpd * bs] == here).astype(F32).astype(BF16)

    landed(inbox, box_recv)
    app = jnp.dot(place[...], inbox[...].reshape(tpd * bs, tile), preferred_element_type=F32)
    applied = jnp.concatenate([app[s * bs : (s + 1) * bs] for s in range(region)], axis=1)

    split = pieces(applied)
    stack = jnp.concatenate([split, basis[...]], axis=0)
    raw = fold(lax.dot_general(split, stack, NT, preferred_element_type=F32), bs)
    raw = jnp.concatenate([raw, jnp.zeros((bs, 64 - 2 * bs - krylov), F32)], axis=1)
    me = r * ncol + c
    tail[me] = jnp.concatenate([raw[: bs // 2], raw[bs // 2 :]], axis=1)

    def give(row, col):
        remote(tail.at[me], tail.at[me], tail_send, tail_recv, {"row": row, "col": col}).start()

    columns = far + near
    for pair in range(0, across, 2):
        for i in range(nrow):
            for k in columns[pair : pair + 2]:
                give(i, k)
    for k in columns[across:]:
        for i in range(nrow):
            give(i, k)
    for i in range(1, nrow):
        give(lax.rem(r + i, nrow), c)

    landed(corr_row, cr_recv)
    corr = jnp.sum(corr_row[...], axis=0) / entries
    corr = jnp.concatenate([corr[:, i * krylov : (i + 1) * krylov] for i in range(folds)], axis=0)[:krylov]
    eye = (
        lax.broadcasted_iota(jnp.int32, (krylov, krylov), 0) == lax.broadcasted_iota(jnp.int32, (krylov, krylov), 1)
    ).astype(F32)
    once = eye - corr
    both = eye + once
    kern = exact(both, eye + exact(once, once)) * (inverse_root / entries * inverse_root)
    before, after = 2 * bs, 64 - 2 * bs - krylov
    down, along = (lax.broadcasted_iota(jnp.int32, (64, bs), d) for d in (0, 1))
    gather = ((down == along) | (down == along + bs)).astype(F32) / entries
    mix = jnp.concatenate(
        [
            jnp.pad(both * inverse_root, ((before, after), (0, 0))),
            gather,
            jnp.zeros((64, 64 + before - krylov - bs), F32),
            jnp.pad(kern, ((before, after), (0, after))),
        ],
        axis=1,
    )
    mix = jnp.concatenate([mix, jnp.zeros((64, 128), F32)], axis=0)
    coarse = mix.astype(BF16).astype(F32)
    mix = jnp.concatenate([coarse, mix - coarse], axis=1).astype(BF16)
    sub = lax.broadcasted_iota(jnp.int32, (bs, 128), 0)
    lane = lax.broadcasted_iota(jnp.int32, (bs, 128), 1)
    right, below = lane >= 64, sub >= bs // 2

    landed(tail, tail_recv)

    sums = [tail[i] for i in range(nrow * ncol)]
    while len(sums) > 1:
        sums = [sum(sums[i : i + 2]) for i in range(0, len(sums), 2)]
    total = sums[0]
    turned = jnp.concatenate([total[:, 64:], total[:, :64]], axis=1)
    total = jnp.where(right == below, jnp.concatenate([total, total], axis=0), jnp.concatenate([turned, turned], axis=0))
    made = fold(jnp.dot(pieces(total), mix, preferred_element_type=F32), bs)
    made = made[:, :128] + made[:, 128:]
    columns = [jnp.zeros((bs, 128), F32)] * bs
    for d in range(bs):
        energy = jnp.where(lane == krylov + lax.rem(sub + d, bs), made, 0.0)
        turned = total if d == 0 else pltpu.roll(total, bs - d, 0)
        gram = jnp.sum(jnp.where(right, -made * turned, energy), axis=1, keepdims=True)
        for j in range(bs):
            if (j - d) % bs >= j:
                columns[j] = jnp.where(sub == (j - d) % bs, gram, columns[j])
    coefficients = made[:, :krylov]
    coef_ref[...] = coefficients

    factor = jnp.zeros((bs, tile), F32)
    inverse = jnp.zeros((bs, tile), F32)
    for j in range(bs):
        root = jnp.broadcast_to(lax.rsqrt(columns[j][j : j + 1]), (bs, tile))
        column = jnp.where(sub >= j, columns[j] * root, 0.0)
        for k in range(j + 1, bs):
            columns[k] = columns[k] - column * column[k : k + 1]
        factor = jnp.where(lane == j, column, factor)
        inverse = jnp.where(sub == j, root, inverse)
        columns[j] = jnp.where(sub > j, column, 0.0)
    factor_ref[...] = factor[:, :bs]

    correction = fold(jnp.dot(pieces(coefficients * inverse_root), basis[...], preferred_element_type=F32), bs)
    steps = [columns[j] * inverse for j in range(bs - 1)]
    for s in range(region):
        part = slice(s * tile, (s + 1) * tile)
        solved = (applied[:, part] - correction[:, part]) * inverse
        for j in range(bs - 1):
            solved = solved - steps[j] * solved[j : j + 1]
        new_ref[:, part] = solved

    for m in range(kinds):
        sent = cols[m].at[pl.ds(0, (nrow - 1) * region)]
        pltpu.make_async_copy(sent, sent, ser_send.at[m]).wait()
    for ref, sem in (
        (seg_in, seg_send), (corr_col, cc_send), (inbox, box_send), (corr_row, cr_send), (tail, tail_send)
    ):
        landed(ref, sem)


def leave(new_ref, coef_ref, factor_ref, new_hbm, coef_hbm, factor_hbm, sem):
    copies = [
        pltpu.make_async_copy(src, dst, sem.at[i])
        for i, (src, dst) in enumerate(((new_ref, new_hbm), (coef_ref, coef_hbm), (factor_ref, factor_hbm)))
    ]
    for copy in copies:
        copy.start()
    for copy in copies:
        copy.wait()


def shards(basis, expand, tiles, tile_rows, tile_cols):
    nrow = lax.axis_size("row")
    ncol = lax.axis_size("col")
    krylov, length = basis.shape
    kinds, tpd, tile, _ = tiles.shape
    bs = expand.shape[1]
    region = length // tile
    cap = tpd // ncol
    width = -(-tpd * bs // 128) * 128
    dma = pltpu.SemaphoreType.DMA
    band = 16
    lanes = -(-(-(-krylov // band) * krylov) // 128) * 128
    vmem, hbm = pl.BlockSpec(memory_space=pltpu.VMEM), pl.BlockSpec(memory_space=pltpu.HBM)
    shapes = (
        jax.ShapeDtypeStruct((bs, length), F32),
        jax.ShapeDtypeStruct((bs, krylov), F32),
        jax.ShapeDtypeStruct((bs, bs), F32),
    )
    held = pl.pallas_call(
        functools.partial(kernel, nrow, ncol),
        out_shape=shapes,
        in_specs=[hbm] * 5,
        out_specs=(vmem, vmem, vmem),
        scratch_shapes=[
            pltpu.VMEM(expand.shape, F32),
            pltpu.SMEM((tpd,), jnp.int32),
            pltpu.SMEM((tpd,), jnp.int32),
            pltpu.VMEM((krylov, length), BF16),
            pltpu.VMEM((kinds, tpd, tile, tile), BF16),
            *[pltpu.VMEM((nrow * region, bs, tile), BF16)] * kinds,
            pltpu.VMEM((ncol, cap * bs, tile), BF16),
            pltpu.VMEM((ncol, cap * bs, tile), BF16),
            pltpu.VMEM((ncol, 1, width), jnp.int32),
            pltpu.VMEM((ncol, 1, width), jnp.int32),
            pltpu.VMEM((ncol, band, lanes), F32),
            pltpu.VMEM((nrow, band, lanes), F32),
            pltpu.VMEM((nrow * ncol, bs // 2, 128), F32),
            pltpu.VMEM((region * bs, tpd * bs), BF16),
            pltpu.VMEM((2, cap * bs, tile), F32),
            dma((3,)),
            dma,
            dma,
            dma((kinds,)),
            dma((kinds, nrow // 2)),
            dma((kinds,)),
        ]
        + [dma] * 10
        + [pltpu.SemaphoreType.REGULAR((max(ncol // 2 - 2, 1),))] * 2,
        compiler_params=pltpu.CompilerParams(
            collective_id=0, has_side_effects=True, vmem_limit_bytes=48 * 1024 * 1024
        ),
    )(*(pltpu.with_memory_space_constraint(x, pltpu.HBM) for x in (expand, tile_rows, tile_cols, basis, tiles)))
    return pl.pallas_call(
        leave,
        out_shape=shapes,
        in_specs=[vmem] * 3,
        out_specs=(hbm, hbm, hbm),
        scratch_shapes=[dma((3,))],
    )(*(pltpu.with_memory_space_constraint(x, pltpu.VMEM) for x in held))


def solution(mesh):
    return jax.shard_map(
        shards,
        mesh=mesh,
        in_specs=(
            P(None, ("row", "col")),
            P(),
            P(None, ("row", "col"), None, None),
            P(("row", "col")),
            P(("row", "col")),
        ),
        out_specs=(P(None, ("row", "col")), P(), P()),
        check_vma=False,
    )
```

```python
import functools
import math

import jax
import jax.numpy as jnp
from jax import lax
from jax.experimental import pallas as pl
from jax.experimental.pallas import tpu as pltpu
from jax.sharding import PartitionSpec as P

F32 = jnp.float32
BF16 = jnp.bfloat16
NT = (((1,), (1,)), ((), ()))


def exact(a, b, dims=(((1,), (0,)), ((), ()))):
    return lax.dot_general(a, b, dims, precision=lax.Precision.HIGHEST, preferred_element_type=F32)


def pieces(x):
    one = x.astype(BF16).astype(F32)
    return jnp.concatenate([one, x - one], axis=0).astype(BF16)


def fold(x, rows):
    return x[:rows] + x[rows:]


def kernel(
    nrow,
    ncol,
    expand_hbm,
    rows_hbm,
    picks_hbm,
    basis_hbm,
    tiles_hbm,
    new_ref,
    coef_ref,
    factor_ref,
    expand_ref,
    rows_ref,
    picks_ref,
    basis,
    tiles,
    cols0,
    cols1,
    cols2,
    outbox,
    inbox,
    seg_out,
    seg_in,
    corr_col,
    corr_row,
    tail,
    place,
    held,
    small_sem,
    basis_sem,
    tile_sem,
    ser_send,
    ser_recv,
    rest_recv,
    seg_send,
    seg_recv,
    box_send,
    box_recv,
    cc_send,
    cc_recv,
    cr_send,
    cr_recv,
    tail_send,
    tail_recv,
    low_sem,
    high_sem,
):
    r = lax.axis_index("row")
    c = lax.axis_index("col")
    cols = (cols0, cols1, cols2)
    krylov, length = basis.shape
    kinds, tpd, tile, _ = tiles.shape
    cap = tpd // ncol
    region = length // tile
    bs = expand_ref.shape[1]
    entries = length * nrow * ncol
    inverse_root = 1.0 / math.sqrt(entries)
    width = seg_in.shape[2]

    parts = 4
    for i in range(parts):
        part = pl.ds(i * (length // parts), length // parts)
        pltpu.make_async_copy(basis_hbm.at[:, part], basis.at[:, part], basis_sem).start()
    small = [
        pltpu.make_async_copy(src, dst, small_sem.at[i])
        for i, (src, dst) in enumerate(((expand_hbm, expand_ref), (rows_hbm, rows_ref), (picks_hbm, picks_ref)))
    ]
    for copy in small:
        copy.start()

    outer = nrow // 2
    side, pair = lax.rem(r, 2), lax.div(r, 2)
    mate = r + 1 - 2 * side
    half = region // 2

    def other(j):
        return 2 * lax.rem(pair + j, outer) + side

    def signal(sem, where):
        pl.semaphore_signal(sem, inc=1, device_id=where, device_id_type=pl.DeviceIdType.MESH)

    barrier = pltpu.get_barrier_semaphore()
    has_low, has_high = c >= 2, c < ncol - 2
    even = c - lax.rem(c, 2)

    def low(i):
        return {"col": lax.rem(even - 2 + i + ncol, ncol)}

    def high(i):
        return {"col": lax.rem(even + 2 + i, ncol)}

    signal(barrier, {"row": mate})
    for j in range(1, outer):
        signal(barrier, {"row": other(j)})
    signal(barrier, {"col": c + 1 - 2 * lax.rem(c, 2)})
    for i in range(2):
        pl.when(has_low)(lambda: signal(barrier, low(i)))
        pl.when(has_high)(lambda: signal(barrier, high(i)))

    def tell(i):
        pl.when(has_low)(lambda: signal(high_sem.at[i], low(lax.rem(c, 2))))
        pl.when(has_high)(lambda: signal(low_sem.at[i], high(lax.rem(c, 2))))

    def hear(i):
        pl.when(has_low)(lambda: pl.semaphore_wait(low_sem.at[i], 1))
        pl.when(has_high)(lambda: pl.semaphore_wait(high_sem.at[i], 1))

    def remote(src, dst, send_sem, recv_sem, where):
        return pltpu.make_async_remote_copy(
            src_ref=src, dst_ref=dst, send_sem=send_sem, recv_sem=recv_sem,
            device_id=where, device_id_type=pl.DeviceIdType.MESH,
        )

    def landed(ref, sem):
        part = ref.at[pl.ds(0, ref.shape[0] - 1)]
        pltpu.make_async_copy(part, part, sem).wait()

    def row_at(j):
        peer = lax.rem(r + j, nrow)
        return peer, {"row": peer}

    def col_at(j):
        peer = lax.rem(c + j, ncol)
        return peer, {"col": peer}

    small[0].wait()
    pltpu.make_async_copy(basis_hbm, basis, basis_sem).wait()
    def make(m):
        one = pieces(expand_ref[m])
        for l in range(region):
            part = jnp.dot(one, basis[:, l * tile : (l + 1) * tile], preferred_element_type=F32)
            cols[m][r * region + l] = fold(part, bs).astype(BF16)

    def block(m, owner, h):
        return cols[m].at[pl.ds(owner * region + h * half, half)]

    def first_half(m, owner, h, peer, slot):
        part = block(m, owner, h)
        return remote(part, part, ser_send.at[m], ser_recv.at[m, slot], {"row": peer})

    def send_rest(m, owner, h, peer):
        part = block(m, owner, h)
        remote(part, part, ser_send.at[m], rest_recv.at[m], {"row": peer}).start()

    def spread(m):
        first_half(m, r, 1, mate, 0).start()
        for j in range(1, outer):
            first_half(m, r, 0, other(j), outer - j).start()

    make(0)

    pl.semaphore_wait(barrier, outer + 1 + 2 * (has_low.astype(jnp.int32) + has_high.astype(jnp.int32)))
    spread(0)
    rounds = ncol // 2 - 2
    if rounds > 0:
        tell(0)

    for m in range(1, kinds):
        make(m)
        spread(m)

    for m in range(kinds):
        send_rest(m, r, 0, mate)
        for j in range(1, outer):
            send_rest(m, r, 1, other(j))

    for m in range(kinds):
        for k in range(ncol):
            part = pl.ds(k * cap, cap)
            pltpu.make_async_copy(tiles_hbm.at[m, part], tiles.at[m, part], tile_sem).start()

    small[1].wait()
    small[2].wait()
    slot = lax.broadcasted_iota(jnp.int32, (1, width), 1)
    entry, inner = lax.rem(lax.div(slot, bs), cap), lax.rem(slot, bs)
    for k in range(ncol):
        line = jnp.zeros((1, width), jnp.int32)
        for t in range(cap):
            line = jnp.where(entry == t, rows_ref[k * cap + t] * bs, line)
        seg_out[k] = line + inner
    seg_in[c] = seg_out[c]

    corr = lax.dot_general(basis[...], basis[...], NT, preferred_element_type=F32)
    band = corr_col.shape[1]
    lanes = corr_col.shape[2]
    folds = -(-krylov // band)
    corr = jnp.pad(corr, ((0, folds * band - krylov), (0, 0)))
    corr_col[c] = jnp.concatenate(
        [corr[i * band : (i + 1) * band] for i in range(folds)] + [jnp.zeros((band, lanes - folds * krylov), F32)], axis=1
    )

    def relay(m):
        first_half(m, mate, 1, mate, 0).wait_recv()
        for j in range(1, outer):
            send_rest(m, mate, 1, other(j))
        for j in range(1, outer):
            first_half(m, other(j), 0, other(j), j).wait_recv()
            send_rest(m, other(j), 0, mate)

    def relayed(m):
        rest = cols[m].at[pl.ds(0, (3 * outer - 2) * half)]
        pltpu.make_async_copy(rest, rest, rest_recv.at[m]).wait()

    relay(0)
    for i in range(rounds - 1):
        hear(i)
        tell(i + 1)
    relay(1)
    if rounds > 0:
        hear(rounds - 1)
    for m in range(2, kinds):
        relay(m)
    for j in range(1, ncol):
        peer, where = col_at(j)
        remote(seg_out.at[peer], seg_in.at[c], seg_send, seg_recv, where).start()
    for j in range(1, ncol):
        peer, where = col_at(j)
        remote(corr_col.at[c], corr_col.at[c], cc_send, cc_recv, where).start()
    for m in range(kinds - 1):
        relayed(m)

    pltpu.make_async_copy(tiles_hbm, tiles, tile_sem).wait()

    def products(k, t, ms):
        out = []
        for g in (k * cap + t, k * cap + t + 1):
            at = picks_ref[g]
            x = jnp.concatenate([cols[m][at] for m in ms], axis=1)
            w = jnp.concatenate([tiles[m, g] for m in ms], axis=1)
            out.append(lax.dot_general(x, w, NT, preferred_element_type=F32))
        return jnp.concatenate(out, axis=0)

    def box_copy(k):
        return remote(outbox.at[k], inbox.at[c], box_send, box_recv, {"col": k})

    across = ncol // 2
    mine = lax.div(c, across)

    upper = mine == 1

    def far_side(i):
        return jnp.where(upper, i, ncol - 2 - 2 * lax.div(i, 2) + lax.rem(i, 2))

    def near_side(i):
        step = jnp.where(lax.rem(c, 2) == 1, i, lax.rem(i, across - 1) + 1)
        return mine * across + lax.rem(c + step, across)

    far = [far_side(jnp.int32(i)) for i in range(across)]
    near = [near_side(jnp.int32(i)) for i in range(1, across)]
    early = held.shape[0]
    for i in range(early):
        for t in range(0, cap, 2):
            held[i, t * bs : (t + 2) * bs] = products(far[i], t, range(kinds - 1))

    relayed(kinds - 1)

    def whole(k, dst):
        for t in range(0, cap, 2):
            dst[k, t * bs : (t + 2) * bs] = products(k, t, range(kinds)).astype(BF16)

    for i in range(early):
        for t in range(0, cap, 2):
            rows = slice(t * bs, (t + 2) * bs)
            outbox[far[i], rows] = (held[i, rows] + products(far[i], t, (kinds - 1,))).astype(BF16)
        box_copy(far[i]).start()

    def pick(s):
        others = across - 2
        k = jnp.where(s < others, near_side(s + 1), near_side(jnp.int32(across - 1)))
        at = s - others + early
        return jnp.where((s >= others) & (at < across), far_side(at), k)

    def send(s, carry):
        k = pick(s)
        whole(k, outbox)
        box_copy(k).start()
        return carry

    lax.fori_loop(0, 2 * across - 1 - early, send, 0)
    whole(c, inbox)

    landed(corr_col, cc_recv)
    corr_row[r] = jnp.sum(corr_col[...], axis=0)
    for j in range(1, nrow):
        peer, where = row_at(j)
        remote(corr_row.at[r], corr_row.at[r], cr_send, cr_recv, where).start()
    landed(seg_in, seg_recv)
    line = seg_in[0]
    for k in range(1, ncol):
        line = jnp.where(lax.div(slot, cap * bs) == k, seg_in[k], line)
    here = lax.broadcasted_iota(jnp.int32, (region * bs, tpd * bs), 0) + c * (region * bs)
    place[...] = (line[:, : tpd * bs] == here).astype(F32).astype(BF16)

    landed(inbox, box_recv)
    app = jnp.dot(place[...], inbox[...].reshape(tpd * bs, tile), preferred_element_type=F32)
    applied = jnp.concatenate([app[s * bs : (s + 1) * bs] for s in range(region)], axis=1)

    split = pieces(applied)
    stack = jnp.concatenate([split, basis[...]], axis=0)
    raw = fold(lax.dot_general(split, stack, NT, preferred_element_type=F32), bs)
    raw = jnp.concatenate([raw, jnp.zeros((bs, 64 - 2 * bs - krylov), F32)], axis=1)
    me = r * ncol + c
    tail[me] = jnp.concatenate([raw[: bs // 2], raw[bs // 2 :]], axis=1)

    def give(row, col):
        remote(tail.at[me], tail.at[me], tail_send, tail_recv, {"row": row, "col": col}).start()

    columns = far + near
    for pair in range(0, across, 2):
        for i in range(nrow):
            for k in columns[pair : pair + 2]:
                give(i, k)
    for k in columns[across:]:
        for i in range(nrow):
            give(i, k)
    for i in range(1, nrow):
        give(lax.rem(r + i, nrow), c)

    landed(corr_row, cr_recv)
    corr = jnp.sum(corr_row[...], axis=0) / entries
    corr = jnp.concatenate([corr[:, i * krylov : (i + 1) * krylov] for i in range(folds)], axis=0)[:krylov]
    eye = (
        lax.broadcasted_iota(jnp.int32, (krylov, krylov), 0) == lax.broadcasted_iota(jnp.int32, (krylov, krylov), 1)
    ).astype(F32)
    once = eye - corr
    both = eye + once
    kern = exact(both, eye + exact(once, once)) * (inverse_root / entries * inverse_root)
    before, after = 2 * bs, 64 - 2 * bs - krylov
    down, along = (lax.broadcasted_iota(jnp.int32, (64, bs), d) for d in (0, 1))
    gather = ((down == along) | (down == along + bs)).astype(F32) / entries
    mix = jnp.concatenate(
        [
            jnp.pad(both * inverse_root, ((before, after), (0, 0))),
            gather,
            jnp.zeros((64, 64 + before - krylov - bs), F32),
            jnp.pad(kern, ((before, after), (0, after))),
        ],
        axis=1,
    )
    mix = jnp.concatenate([mix, jnp.zeros((64, 128), F32)], axis=0)
    coarse = mix.astype(BF16).astype(F32)
    mix = jnp.concatenate([coarse, mix - coarse], axis=1).astype(BF16)
    sub = lax.broadcasted_iota(jnp.int32, (bs, 128), 0)
    lane = lax.broadcasted_iota(jnp.int32, (bs, 128), 1)
    right, below = lane >= 64, sub >= bs // 2

    landed(tail, tail_recv)

    sums = [tail[i] for i in range(nrow * ncol)]
    while len(sums) > 1:
        sums = [sum(sums[i : i + 2]) for i in range(0, len(sums), 2)]
    total = sums[0]
    turned = jnp.concatenate([total[:, 64:], total[:, :64]], axis=1)
    total = jnp.where(right == below, jnp.concatenate([total, total], axis=0), jnp.concatenate([turned, turned], axis=0))
    made = fold(jnp.dot(pieces(total), mix, preferred_element_type=F32), bs)
    made = made[:, :128] + made[:, 128:]
    columns = [jnp.zeros((bs, 128), F32)] * bs
    for d in range(bs):
        energy = jnp.where(lane == krylov + lax.rem(sub + d, bs), made, 0.0)
        turned = total if d == 0 else pltpu.roll(total, bs - d, 0)
        gram = jnp.sum(jnp.where(right, -made * turned, energy), axis=1, keepdims=True)
        for j in range(bs):
            if (j - d) % bs >= j:
                columns[j] = jnp.where(sub == (j - d) % bs, gram, columns[j])
    coefficients = made[:, :krylov]
    coef_ref[...] = coefficients

    factor = jnp.zeros((bs, tile), F32)
    inverse = jnp.zeros((bs, tile), F32)
    for j in range(bs):
        root = jnp.broadcast_to(lax.rsqrt(columns[j][j : j + 1]), (bs, tile))
        column = jnp.where(sub >= j, columns[j] * root, 0.0)
        for k in range(j + 1, bs):
            columns[k] = columns[k] - column * column[k : k + 1]
        factor = jnp.where(lane == j, column, factor)
        inverse = jnp.where(sub == j, root, inverse)
        columns[j] = jnp.where(sub > j, column, 0.0)
    factor_ref[...] = factor[:, :bs]

    correction = fold(jnp.dot(pieces(coefficients * inverse_root), basis[...], preferred_element_type=F32), bs)
    steps = [columns[j] * inverse for j in range(bs - 1)]
    for s in range(region):
        part = slice(s * tile, (s + 1) * tile)
        solved = (applied[:, part] - correction[:, part]) * inverse
        for j in range(bs - 1):
            solved = solved - steps[j] * solved[j : j + 1]
        new_ref[:, part] = solved

    for m in range(kinds):
        sent = cols[m].at[pl.ds(0, (nrow - 1) * region)]
        pltpu.make_async_copy(sent, sent, ser_send.at[m]).wait()
    for ref, sem in (
        (seg_in, seg_send), (corr_col, cc_send), (inbox, box_send), (corr_row, cr_send), (tail, tail_send)
    ):
        landed(ref, sem)


def leave(new_ref, coef_ref, factor_ref, new_hbm, coef_hbm, factor_hbm, sem):
    copies = [
        pltpu.make_async_copy(src, dst, sem.at[i])
        for i, (src, dst) in enumerate(((new_ref, new_hbm), (coef_ref, coef_hbm), (factor_ref, factor_hbm)))
    ]
    for copy in copies:
        copy.start()
    for copy in copies:
        copy.wait()


def shards(basis, expand, tiles, tile_rows, tile_cols):
    nrow = lax.axis_size("row")
    ncol = lax.axis_size("col")
    krylov, length = basis.shape
    kinds, tpd, tile, _ = tiles.shape
    bs = expand.shape[1]
    region = length // tile
    cap = tpd // ncol
    width = -(-tpd * bs // 128) * 128
    dma = pltpu.SemaphoreType.DMA
    band = 16
    lanes = -(-(-(-krylov // band) * krylov) // 128) * 128
    vmem, hbm = pl.BlockSpec(memory_space=pltpu.VMEM), pl.BlockSpec(memory_space=pltpu.HBM)
    shapes = (
        jax.ShapeDtypeStruct((bs, length), F32),
        jax.ShapeDtypeStruct((bs, krylov), F32),
        jax.ShapeDtypeStruct((bs, bs), F32),
    )
    held = pl.pallas_call(
        functools.partial(kernel, nrow, ncol),
        out_shape=shapes,
        in_specs=[hbm] * 5,
        out_specs=(vmem, vmem, vmem),
        scratch_shapes=[
            pltpu.VMEM(expand.shape, F32),
            pltpu.SMEM((tpd,), jnp.int32),
            pltpu.SMEM((tpd,), jnp.int32),
            pltpu.VMEM((krylov, length), BF16),
            pltpu.VMEM((kinds, tpd, tile, tile), BF16),
            *[pltpu.VMEM((nrow * region, bs, tile), BF16)] * kinds,
            pltpu.VMEM((ncol, cap * bs, tile), BF16),
            pltpu.VMEM((ncol, cap * bs, tile), BF16),
            pltpu.VMEM((ncol, 1, width), jnp.int32),
            pltpu.VMEM((ncol, 1, width), jnp.int32),
            pltpu.VMEM((ncol, band, lanes), F32),
            pltpu.VMEM((nrow, band, lanes), F32),
            pltpu.VMEM((nrow * ncol, bs // 2, 128), F32),
            pltpu.VMEM((region * bs, tpd * bs), BF16),
            pltpu.VMEM((2, cap * bs, tile), F32),
            dma((3,)),
            dma,
            dma,
            dma((kinds,)),
            dma((kinds, nrow // 2)),
            dma((kinds,)),
        ]
        + [dma] * 10
        + [pltpu.SemaphoreType.REGULAR((max(ncol // 2 - 2, 1),))] * 2,
        compiler_params=pltpu.CompilerParams(
            collective_id=0, has_side_effects=True, vmem_limit_bytes=48 * 1024 * 1024
        ),
    )(*(pltpu.with_memory_space_constraint(x, pltpu.HBM) for x in (expand, tile_rows, tile_cols, basis, tiles)))
    return pl.pallas_call(
        leave,
        out_shape=shapes,
        in_specs=[vmem] * 3,
        out_specs=(hbm, hbm, hbm),
        scratch_shapes=[dma((3,))],
    )(*(pltpu.with_memory_space_constraint(x, pltpu.VMEM) for x in held))


def solution(mesh):
    return jax.shard_map(
        shards,
        mesh=mesh,
        in_specs=(
            P(None, ("row", "col")),
            P(),
            P(None, ("row", "col"), None, None),
            P(("row", "col")),
            P(("row", "col")),
        ),
        out_specs=(P(None, ("row", "col")), P(), P()),
        check_vma=False,
    )
```

```python
import functools
import math

import jax
import jax.numpy as jnp
from jax import lax
from jax.experimental import pallas as pl
from jax.experimental.pallas import tpu as pltpu
from jax.sharding import PartitionSpec as P

F32 = jnp.float32
BF16 = jnp.bfloat16
NT = (((1,), (1,)), ((), ()))


def exact(a, b, dims=(((1,), (0,)), ((), ()))):
    return lax.dot_general(a, b, dims, precision=lax.Precision.HIGHEST, preferred_element_type=F32)


def pieces(x):
    one = x.astype(BF16).astype(F32)
    return jnp.concatenate([one, x - one], axis=0).astype(BF16)


def fold(x, rows):
    return x[:rows] + x[rows:]


def kernel(
    nrow,
    ncol,
    expand_hbm,
    rows_hbm,
    picks_hbm,
    basis_hbm,
    tiles_hbm,
    new_ref,
    coef_ref,
    factor_ref,
    expand_ref,
    rows_ref,
    picks_ref,
    basis,
    tiles,
    cols0,
    cols1,
    cols2,
    outbox,
    inbox,
    seg_out,
    seg_in,
    corr_col,
    corr_row,
    tail,
    place,
    held,
    small_sem,
    basis_sem,
    tile_sem,
    ser_send,
    ser_recv,
    rest_recv,
    seg_send,
    seg_recv,
    box_send,
    box_recv,
    cc_send,
    cc_recv,
    cr_send,
    cr_recv,
    tail_send,
    tail_recv,
    low_sem,
    high_sem,
):
    r = lax.axis_index("row")
    c = lax.axis_index("col")
    cols = (cols0, cols1, cols2)
    krylov, length = basis.shape
    kinds, tpd, tile, _ = tiles.shape
    cap = tpd // ncol
    region = length // tile
    bs = expand_ref.shape[1]
    entries = length * nrow * ncol
    inverse_root = 1.0 / math.sqrt(entries)
    width = seg_in.shape[2]

    parts = 4
    for i in range(parts):
        part = pl.ds(i * (length // parts), length // parts)
        pltpu.make_async_copy(basis_hbm.at[:, part], basis.at[:, part], basis_sem).start()
    small = [
        pltpu.make_async_copy(src, dst, small_sem.at[i])
        for i, (src, dst) in enumerate(((expand_hbm, expand_ref), (rows_hbm, rows_ref), (picks_hbm, picks_ref)))
    ]
    for copy in small:
        copy.start()

    outer = nrow // 2
    side, pair = lax.rem(r, 2), lax.div(r, 2)
    mate = r + 1 - 2 * side
    half = region // 2

    def other(j):
        return 2 * lax.rem(pair + j, outer) + side

    def signal(sem, where):
        pl.semaphore_signal(sem, inc=1, device_id=where, device_id_type=pl.DeviceIdType.MESH)

    barrier = pltpu.get_barrier_semaphore()
    has_low, has_high = c >= 2, c < ncol - 2
    even = c - lax.rem(c, 2)

    def low(i):
        return {"col": lax.rem(even - 2 + i + ncol, ncol)}

    def high(i):
        return {"col": lax.rem(even + 2 + i, ncol)}

    signal(barrier, {"row": mate})
    for j in range(1, outer):
        signal(barrier, {"row": other(j)})
    signal(barrier, {"col": c + 1 - 2 * lax.rem(c, 2)})
    for i in range(2):
        pl.when(has_low)(lambda: signal(barrier, low(i)))
        pl.when(has_high)(lambda: signal(barrier, high(i)))

    def tell(i):
        pl.when(has_low)(lambda: signal(high_sem.at[i], low(lax.rem(c, 2))))
        pl.when(has_high)(lambda: signal(low_sem.at[i], high(lax.rem(c, 2))))

    def hear(i):
        pl.when(has_low)(lambda: pl.semaphore_wait(low_sem.at[i], 1))
        pl.when(has_high)(lambda: pl.semaphore_wait(high_sem.at[i], 1))

    def remote(src, dst, send_sem, recv_sem, where):
        return pltpu.make_async_remote_copy(
            src_ref=src, dst_ref=dst, send_sem=send_sem, recv_sem=recv_sem,
            device_id=where, device_id_type=pl.DeviceIdType.MESH,
        )

    def landed(ref, sem):
        part = ref.at[pl.ds(0, ref.shape[0] - 1)]
        pltpu.make_async_copy(part, part, sem).wait()

    def row_at(j):
        peer = lax.rem(r + j, nrow)
        return peer, {"row": peer}

    def col_at(j):
        peer = lax.rem(c + j, ncol)
        return peer, {"col": peer}

    small[0].wait()
    pltpu.make_async_copy(basis_hbm, basis, basis_sem).wait()
    def make(m):
        one = pieces(expand_ref[m])
        for l in range(region):
            part = jnp.dot(one, basis[:, l * tile : (l + 1) * tile], preferred_element_type=F32)
            cols[m][r * region + l] = fold(part, bs).astype(BF16)

    def block(m, owner, h):
        return cols[m].at[pl.ds(owner * region + h * half, half)]

    def first_half(m, owner, h, peer, slot):
        part = block(m, owner, h)
        return remote(part, part, ser_send.at[m], ser_recv.at[m, slot], {"row": peer})

    def send_rest(m, owner, h, peer):
        part = block(m, owner, h)
        remote(part, part, ser_send.at[m], rest_recv.at[m], {"row": peer}).start()

    def spread(m):
        first_half(m, r, 1, mate, 0).start()
        for j in range(1, outer):
            first_half(m, r, 0, other(j), outer - j).start()

    make(0)

    pl.semaphore_wait(barrier, outer + 1 + 2 * (has_low.astype(jnp.int32) + has_high.astype(jnp.int32)))
    spread(0)
    rounds = ncol // 2 - 2
    if rounds > 0:
        tell(0)

    for m in range(1, kinds):
        make(m)
        spread(m)

    for m in range(kinds):
        send_rest(m, r, 0, mate)
        for j in range(1, outer):
            send_rest(m, r, 1, other(j))

    for m in range(kinds):
        for k in range(ncol):
            part = pl.ds(k * cap, cap)
            pltpu.make_async_copy(tiles_hbm.at[m, part], tiles.at[m, part], tile_sem).start()

    small[1].wait()
    small[2].wait()
    slot = lax.broadcasted_iota(jnp.int32, (1, width), 1)
    entry, inner = lax.rem(lax.div(slot, bs), cap), lax.rem(slot, bs)
    for k in range(ncol):
        line = jnp.zeros((1, width), jnp.int32)
        for t in range(cap):
            line = jnp.where(entry == t, rows_ref[k * cap + t] * bs, line)
        seg_out[k] = line + inner
    seg_in[c] = seg_out[c]

    corr = lax.dot_general(basis[...], basis[...], NT, preferred_element_type=F32)
    band = corr_col.shape[1]
    lanes = corr_col.shape[2]
    folds = -(-krylov // band)
    corr = jnp.pad(corr, ((0, folds * band - krylov), (0, 0)))
    corr_col[c] = jnp.concatenate(
        [corr[i * band : (i + 1) * band] for i in range(folds)] + [jnp.zeros((band, lanes - folds * krylov), F32)], axis=1
    )

    def relay(m):
        first_half(m, mate, 1, mate, 0).wait_recv()
        for j in range(1, outer):
            send_rest(m, mate, 1, other(j))
        for j in range(1, outer):
            first_half(m, other(j), 0, other(j), j).wait_recv()
            send_rest(m, other(j), 0, mate)

    def relayed(m):
        rest = cols[m].at[pl.ds(0, (3 * outer - 2) * half)]
        pltpu.make_async_copy(rest, rest, rest_recv.at[m]).wait()

    relay(0)
    for i in range(rounds - 1):
        hear(i)
        tell(i + 1)
    relay(1)
    if rounds > 0:
        hear(rounds - 1)
    for m in range(2, kinds):
        relay(m)
    for j in range(1, ncol):
        peer, where = col_at(j)
        remote(seg_out.at[peer], seg_in.at[c], seg_send, seg_recv, where).start()
    for j in range(1, ncol):
        peer, where = col_at(j)
        remote(corr_col.at[c], corr_col.at[c], cc_send, cc_recv, where).start()
    for m in range(kinds - 1):
        relayed(m)

    pltpu.make_async_copy(tiles_hbm, tiles, tile_sem).wait()

    def products(k, t, ms):
        out = []
        for g in (k * cap + t, k * cap + t + 1):
            at = picks_ref[g]
            x = jnp.concatenate([cols[m][at] for m in ms], axis=1)
            w = jnp.concatenate([tiles[m, g] for m in ms], axis=1)
            out.append(lax.dot_general(x, w, NT, preferred_element_type=F32))
        return jnp.concatenate(out, axis=0)

    def box_copy(k):
        return remote(outbox.at[k], inbox.at[c], box_send, box_recv, {"col": k})

    across = ncol // 2
    mine = lax.div(c, across)

    upper = mine == 1

    def far_side(i):
        return jnp.where(upper, i, ncol - 2 - 2 * lax.div(i, 2) + lax.rem(i, 2))

    def near_side(i):
        step = jnp.where(lax.rem(c, 2) == 1, i, lax.rem(i, across - 1) + 1)
        return mine * across + lax.rem(c + step, across)

    far = [far_side(jnp.int32(i)) for i in range(across)]
    near = [near_side(jnp.int32(i)) for i in range(1, across)]
    early = held.shape[0]
    for i in range(early):
        for t in range(0, cap, 2):
            held[i, t * bs : (t + 2) * bs] = products(far[i], t, range(kinds - 1))

    relayed(kinds - 1)

    def whole(k, dst):
        for t in range(0, cap, 2):
            dst[k, t * bs : (t + 2) * bs] = products(k, t, range(kinds)).astype(BF16)

    for i in range(early):
        for t in range(0, cap, 2):
            rows = slice(t * bs, (t + 2) * bs)
            outbox[far[i], rows] = (held[i, rows] + products(far[i], t, (kinds - 1,))).astype(BF16)
        box_copy(far[i]).start()

    def pick(s):
        others = across - 2
        first = s == 0
        at = jnp.where(first, early, s - others + early)
        k = near_side(jnp.where(s <= others, jnp.maximum(s, 1), across - 1))
        return jnp.where(first | ((s > others) & (at < across)), far_side(at), k)

    def send(s, carry):
        k = pick(s)
        whole(k, outbox)
        box_copy(k).start()
        return carry

    lax.fori_loop(0, 2 * across - 1 - early, send, 0)
    whole(c, inbox)

    landed(corr_col, cc_recv)
    corr_row[r] = jnp.sum(corr_col[...], axis=0)
    for j in range(1, nrow):
        peer, where = row_at(j)
        remote(corr_row.at[r], corr_row.at[r], cr_send, cr_recv, where).start()
    landed(seg_in, seg_recv)
    line = seg_in[0]
    for k in range(1, ncol):
        line = jnp.where(lax.div(slot, cap * bs) == k, seg_in[k], line)
    here = lax.broadcasted_iota(jnp.int32, (region * bs, tpd * bs), 0) + c * (region * bs)
    place[...] = (line[:, : tpd * bs] == here).astype(F32).astype(BF16)

    landed(inbox, box_recv)
    app = jnp.dot(place[...], inbox[...].reshape(tpd * bs, tile), preferred_element_type=F32)
    applied = jnp.concatenate([app[s * bs : (s + 1) * bs] for s in range(region)], axis=1)

    split = pieces(applied)
    stack = jnp.concatenate([split, basis[...]], axis=0)
    raw = fold(lax.dot_general(split, stack, NT, preferred_element_type=F32), bs)
    raw = jnp.concatenate([raw, jnp.zeros((bs, 64 - 2 * bs - krylov), F32)], axis=1)
    me = r * ncol + c
    tail[me] = jnp.concatenate([raw[: bs // 2], raw[bs // 2 :]], axis=1)

    def give(row, col):
        remote(tail.at[me], tail.at[me], tail_send, tail_recv, {"row": row, "col": col}).start()

    columns = far + near
    for pair in range(0, across, 2):
        for i in range(nrow):
            for k in columns[pair : pair + 2]:
                give(i, k)
    for k in columns[across:]:
        for i in range(nrow):
            give(i, k)
    for i in range(1, nrow):
        give(lax.rem(r + i, nrow), c)

    landed(corr_row, cr_recv)
    corr = jnp.sum(corr_row[...], axis=0) / entries
    corr = jnp.concatenate([corr[:, i * krylov : (i + 1) * krylov] for i in range(folds)], axis=0)[:krylov]
    eye = (
        lax.broadcasted_iota(jnp.int32, (krylov, krylov), 0) == lax.broadcasted_iota(jnp.int32, (krylov, krylov), 1)
    ).astype(F32)
    once = eye - corr
    both = eye + once
    kern = exact(both, eye + exact(once, once)) * (inverse_root / entries * inverse_root)
    before, after = 2 * bs, 64 - 2 * bs - krylov
    down, along = (lax.broadcasted_iota(jnp.int32, (64, bs), d) for d in (0, 1))
    gather = ((down == along) | (down == along + bs)).astype(F32) / entries
    mix = jnp.concatenate(
        [
            jnp.pad(both * inverse_root, ((before, after), (0, 0))),
            gather,
            jnp.zeros((64, 64 + before - krylov - bs), F32),
            jnp.pad(kern, ((before, after), (0, after))),
        ],
        axis=1,
    )
    mix = jnp.concatenate([mix, jnp.zeros((64, 128), F32)], axis=0)
    coarse = mix.astype(BF16).astype(F32)
    mix = jnp.concatenate([coarse, mix - coarse], axis=1).astype(BF16)
    sub = lax.broadcasted_iota(jnp.int32, (bs, 128), 0)
    lane = lax.broadcasted_iota(jnp.int32, (bs, 128), 1)
    right, below = lane >= 64, sub >= bs // 2

    landed(tail, tail_recv)

    sums = [tail[i] for i in range(nrow * ncol)]
    while len(sums) > 1:
        sums = [sum(sums[i : i + 2]) for i in range(0, len(sums), 2)]
    total = sums[0]
    turned = jnp.concatenate([total[:, 64:], total[:, :64]], axis=1)
    total = jnp.where(right == below, jnp.concatenate([total, total], axis=0), jnp.concatenate([turned, turned], axis=0))
    made = fold(jnp.dot(pieces(total), mix, preferred_element_type=F32), bs)
    made = made[:, :128] + made[:, 128:]
    columns = [jnp.zeros((bs, 128), F32)] * bs
    for d in range(bs):
        energy = jnp.where(lane == krylov + lax.rem(sub + d, bs), made, 0.0)
        turned = total if d == 0 else pltpu.roll(total, bs - d, 0)
        gram = jnp.sum(jnp.where(right, -made * turned, energy), axis=1, keepdims=True)
        for j in range(bs):
            if (j - d) % bs >= j:
                columns[j] = jnp.where(sub == (j - d) % bs, gram, columns[j])
    coefficients = made[:, :krylov]
    coef_ref[...] = coefficients

    factor = jnp.zeros((bs, tile), F32)
    inverse = jnp.zeros((bs, tile), F32)
    for j in range(bs):
        root = jnp.broadcast_to(lax.rsqrt(columns[j][j : j + 1]), (bs, tile))
        column = jnp.where(sub >= j, columns[j] * root, 0.0)
        for k in range(j + 1, bs):
            columns[k] = columns[k] - column * column[k : k + 1]
        factor = jnp.where(lane == j, column, factor)
        inverse = jnp.where(sub == j, root, inverse)
        columns[j] = jnp.where(sub > j, column, 0.0)
    factor_ref[...] = factor[:, :bs]

    correction = fold(jnp.dot(pieces(coefficients * inverse_root), basis[...], preferred_element_type=F32), bs)
    steps = [columns[j] * inverse for j in range(bs - 1)]
    for s in range(region):
        part = slice(s * tile, (s + 1) * tile)
        solved = (applied[:, part] - correction[:, part]) * inverse
        for j in range(bs - 1):
            solved = solved - steps[j] * solved[j : j + 1]
        new_ref[:, part] = solved

    for m in range(kinds):
        sent = cols[m].at[pl.ds(0, (nrow - 1) * region)]
        pltpu.make_async_copy(sent, sent, ser_send.at[m]).wait()
    for ref, sem in (
        (seg_in, seg_send), (corr_col, cc_send), (inbox, box_send), (corr_row, cr_send), (tail, tail_send)
    ):
        landed(ref, sem)


def leave(new_ref, coef_ref, factor_ref, new_hbm, coef_hbm, factor_hbm, sem):
    copies = [
        pltpu.make_async_copy(src, dst, sem.at[i])
        for i, (src, dst) in enumerate(((new_ref, new_hbm), (coef_ref, coef_hbm), (factor_ref, factor_hbm)))
    ]
    for copy in copies:
        copy.start()
    for copy in copies:
        copy.wait()


def shards(basis, expand, tiles, tile_rows, tile_cols):
    nrow = lax.axis_size("row")
    ncol = lax.axis_size("col")
    krylov, length = basis.shape
    kinds, tpd, tile, _ = tiles.shape
    bs = expand.shape[1]
    region = length // tile
    cap = tpd // ncol
    width = -(-tpd * bs // 128) * 128
    dma = pltpu.SemaphoreType.DMA
    band = 16
    lanes = -(-(-(-krylov // band) * krylov) // 128) * 128
    vmem, hbm = pl.BlockSpec(memory_space=pltpu.VMEM), pl.BlockSpec(memory_space=pltpu.HBM)
    shapes = (
        jax.ShapeDtypeStruct((bs, length), F32),
        jax.ShapeDtypeStruct((bs, krylov), F32),
        jax.ShapeDtypeStruct((bs, bs), F32),
    )
    held = pl.pallas_call(
        functools.partial(kernel, nrow, ncol),
        out_shape=shapes,
        in_specs=[hbm] * 5,
        out_specs=(vmem, vmem, vmem),
        scratch_shapes=[
            pltpu.VMEM(expand.shape, F32),
            pltpu.SMEM((tpd,), jnp.int32),
            pltpu.SMEM((tpd,), jnp.int32),
            pltpu.VMEM((krylov, length), BF16),
            pltpu.VMEM((kinds, tpd, tile, tile), BF16),
            *[pltpu.VMEM((nrow * region, bs, tile), BF16)] * kinds,
            pltpu.VMEM((ncol, cap * bs, tile), BF16),
            pltpu.VMEM((ncol, cap * bs, tile), BF16),
            pltpu.VMEM((ncol, 1, width), jnp.int32),
            pltpu.VMEM((ncol, 1, width), jnp.int32),
            pltpu.VMEM((ncol, band, lanes), F32),
            pltpu.VMEM((nrow, band, lanes), F32),
            pltpu.VMEM((nrow * ncol, bs // 2, 128), F32),
            pltpu.VMEM((region * bs, tpd * bs), BF16),
            pltpu.VMEM((2, cap * bs, tile), F32),
            dma((3,)),
            dma,
            dma,
            dma((kinds,)),
            dma((kinds, nrow // 2)),
            dma((kinds,)),
        ]
        + [dma] * 10
        + [pltpu.SemaphoreType.REGULAR((max(ncol // 2 - 2, 1),))] * 2,
        compiler_params=pltpu.CompilerParams(
            collective_id=0, has_side_effects=True, vmem_limit_bytes=48 * 1024 * 1024
        ),
    )(*(pltpu.with_memory_space_constraint(x, pltpu.HBM) for x in (expand, tile_rows, tile_cols, basis, tiles)))
    return pl.pallas_call(
        leave,
        out_shape=shapes,
        in_specs=[vmem] * 3,
        out_specs=(hbm, hbm, hbm),
        scratch_shapes=[dma((3,))],
    )(*(pltpu.with_memory_space_constraint(x, pltpu.VMEM) for x in held))


def solution(mesh):
    return jax.shard_map(
        shards,
        mesh=mesh,
        in_specs=(
            P(None, ("row", "col")),
            P(),
            P(None, ("row", "col"), None, None),
            P(("row", "col")),
            P(("row", "col")),
        ),
        out_specs=(P(None, ("row", "col")), P(), P()),
        check_vma=False,
    )
```
